32 devices in a mesh: dp: 16 (over z, y, x), seq: 2 (over core).
Axes of the slice: x: 2, y: 2, z: 4, core: 2. Of those that a mesh axis runs over, the one named last changes fastest.
Arguments:
- activations: bfloat16 [4096, 8192], P(('dp', 'seq')), may hold values from -6 to 6
- queries: bfloat16 [4096, 8192], P(('dp', 'seq')), may hold values from -180 to 180
- keys: bfloat16 [4096, 1024], P(('dp', 'seq')), may hold values from -6 to 6
- out_grad: bfloat16 [4096, 8192], P(('dp', 'seq')), may hold values from -0.078125 to 0.078125
- layout: int32 [8192], replicated, may hold values from 0 to 8191, each once
Outputs:
- value_weight_grad: float32 [8192, 1024], P(('dp', 'seq'))
The draws below stay inside these ranges and needn't reach their ends.
Inputs may be any that keep to these rules, and one draw needn't show every extreme that they name: `layout`: every row number 0 to 8191 appears exactly once.
All inputs are finite; a program needn't handle non-finite values.
Results may differ from the reference program's by a relative error of at most 0.0049.
Values may be sent and summed in bfloat16 or wider, within the bound.
A program may use at most 128 MiB of HBM per device.

```python
import jax
import jax.numpy as jnp
from jax import lax

D = 8192
H = 64
KVH = 8
HD = 128
LENGTH = 256
TOKENS = 4096


def draw_pair(key):
    base_keys = jnp.clip(jax.random.normal(jax.random.fold_in(key, 11), (TOKENS, KVH * HD), jnp.float32), -6.0, 6.0)
    fresh = jnp.clip(jax.random.normal(jax.random.fold_in(key, 12), (TOKENS, H * HD), jnp.float32), -6.0, 6.0)
    return (fresh, base_keys)


def draw_queries(key, part):
    return draw_pair(key)[0].astype(jnp.bfloat16)


def draw_keys(key, part):
    return draw_pair(key)[1].astype(jnp.bfloat16)


def raised(result, own_key, source, target, blocks, factor):
    owner, partner = [(jnp.arange(result.shape[position]) // (result.shape[position] // blocks)).reshape([-1 if axis == position else 1 for axis in range(result.ndim)]) for position in (source, target)]
    chosen = jax.random.permutation(own_key, blocks)[partner]
    strong = (owner == chosen) | (owner == (partner + blocks // 2) % blocks)
    return jnp.where(strong, factor * result, result)


def block_scale(own_key, dims, split, smallest, high):
    gain, own = 1.0, jax.random.fold_in(own_key, 6)
    for dim, parts in split:
        draws = jnp.exp(jax.random.uniform(jax.random.fold_in(own, dim), (parts,), jnp.float32, smallest / len(split), high / len(split)))
        gain = gain * jnp.repeat(draws, dims[dim] // parts).reshape([-1 if axis == dim else 1 for axis in range(len(dims))])
    return gain


def bell_draw(own_key, extent, spread, limit, shards=(), kind=jnp.bfloat16):
    drawn = spread * jax.random.normal(own_key, extent, jnp.float32)
    if shards:
        drawn = drawn * block_scale(own_key, extent, shards, -0.22, 0.18)
    return jnp.clip(drawn, -limit, limit).astype(kind)


def gaussian_with(rng, extent, width, reach, cuts, heavy, held_as=jnp.bfloat16):
    array = width * jax.random.normal(rng, extent, jnp.float32)
    if cuts:
        array = array * block_scale(rng, extent, cuts, -0.22, 0.18)
    return jnp.clip(raised(array, jax.random.fold_in(rng, 3), *heavy), -reach, reach).astype(held_as)


def setup_inputs(seed: int = 0) -> dict:
    streams_of = jax.random.split(jax.random.key(seed), 6)
    activations = gaussian_with(streams_of[0], (TOKENS, D), 1.0, 6.0, ((0, 32),), (0, 1, 32, 2.75))
    queries = draw_queries(jax.random.fold_in(streams_of[5], 71), 0)
    keys = draw_keys(jax.random.fold_in(streams_of[5], 71), 0)
    out_grad = bell_draw(streams_of[3], (TOKENS, H * HD), ((8 * TOKENS) ** -0.5), 0.078125, ((0, 32),))
    layout = jax.random.permutation(streams_of[4], D).astype(jnp.int32)
    return {"activations": activations, "queries": queries, "keys": keys, "out_grad": out_grad, "layout": layout}


def value_grads(seq_queries, seq_keys, seq_grads):
    length = seq_queries.shape[0]
    per_group = H // KVH
    inv_root = 1.0 / float(HD) ** 0.5
    places = jnp.arange(length)
    allowed = places[:, None] >= places[None, :]
    pieces = []
    for group_index in range(KVH):
        offset = group_index * per_group * HD
        query_block = seq_queries[:, offset:offset + per_group * HD].reshape(length, per_group, HD).astype(jnp.float32)
        grad_block = seq_grads[:, offset:offset + per_group * HD].reshape(length, per_group, HD).astype(jnp.float32)
        key_block = seq_keys[:, group_index * HD:(group_index + 1) * HD].astype(jnp.float32)
        scores = jnp.einsum("igd,jd->gij", query_block, key_block) * inv_root
        scores = jnp.where(allowed[None], scores, -jnp.inf)
        weights = lax.optimization_barrier(jax.nn.softmax(scores, axis=-1).astype(jnp.bfloat16))
        pieces.append(jnp.einsum("gij,igd->jd", weights.astype(jnp.float32), grad_block))
    return jnp.concatenate(pieces, axis=1)


def reference(activations, queries, keys, out_grad, layout):
    count_seqs = activations.shape[0] // LENGTH

    def add_sequence(seq_number, grand_sum):
        first_row = (seq_number * LENGTH).astype(jnp.int32)
        seq_rows = lax.dynamic_slice_in_dim(activations, first_row, LENGTH, 0)
        seq_queries = lax.dynamic_slice_in_dim(queries, first_row, LENGTH, 0)
        seq_keys = lax.dynamic_slice_in_dim(keys, first_row, LENGTH, 0)
        seq_grads = lax.dynamic_slice_in_dim(out_grad, first_row, LENGTH, 0)
        value_grad = value_grads(seq_queries, seq_keys, seq_grads).astype(jnp.bfloat16)
        columns = jnp.take(seq_rows, layout.astype(jnp.int32), axis=1)
        row_term = jnp.dot(columns.T, value_grad, preferred_element_type=jnp.float32)
        row_term = lax.optimization_barrier(row_term.astype(jnp.bfloat16))
        return grand_sum + row_term.astype(jnp.float32)

    return lax.fori_loop(0, count_seqs, add_sequence, jnp.zeros((D, KVH * HD), jnp.float32))
```

```python
import functools
import math

import jax
import jax.numpy as jnp
from jax import lax
from jax.experimental import pallas as pl
from jax.experimental.pallas import tpu as pltpu
from jax.sharding import PartitionSpec as P

H = 64
KVH = 8
HD = 128
SEQ = 2
CHUNK = 256
MESH = pl.DeviceIdType.MESH


def relative(place, step, bits):
    total = 0
    for b in range(bits):
        total = total + (place // (1 << b) + step // (1 << b)) % 2 * (1 << b)
    return total


def turn(z, k, count):
    above = count - 1 - z
    sign = jnp.where(above >= z, 1, -1)
    big, small = jnp.maximum(above, z), jnp.minimum(above, z)
    later = k - (big - small)
    lone = later < 0
    distance = jnp.where(lone, big - k, small - later // 2)
    side = jnp.where(lone | (later % 2 == 1), sign, -sign)
    return z + side * distance


def fused_kernel(
    act_hbm, q_hbm, k_hbm, grad_hbm, layout_hbm, out_ref,
    act, flipped, picked, lay, qb, kb, gb, send, held, vg, down_in, up_in, part, acc,
    load_sem, swap_send, swap_recv, a2a_send, a2a_recv, ag_send, ag_recv,
    fwd_send, fwd_recv, rs_send, up_sem, down_sem, *, planes, inner,
):
    tokens, width = act_hbm.shape
    rows = out_ref.shape[0]
    bits = inner.bit_length() - 1
    me, core = lax.axis_index("dp"), lax.axis_index("seq")
    z, p = me // inner, me % inner
    other = 1 - core
    heads_cols, key_cols = q_hbm.shape[1] // SEQ, k_hbm.shape[1] // SEQ
    length = SEQ * tokens
    per_group = H // KVH
    chunks_core = key_cols // CHUNK
    chunks = SEQ * chunks_core
    place = p * SEQ + core

    loads = [
        pltpu.make_async_copy(act_hbm, act, load_sem.at[0]),
        pltpu.make_async_copy(layout_hbm, lay, load_sem.at[1]),
    ]
    for i, (source, target, cols) in enumerate(
        ((k_hbm, kb, key_cols), (q_hbm, qb, heads_cols), (grad_hbm, gb, heads_cols))
    ):
        loads.append(
            pltpu.make_async_copy(
                source.at[:, pl.ds(pl.multiple_of(core * cols, 128), cols)],
                target.at[pl.ds(pl.multiple_of(core * tokens, 128), tokens), :],
                load_sem.at[2 + i],
            )
        )
    for load in loads:
        load.start()

    barrier = pltpu.get_barrier_semaphore()
    for j in range(1, inner * SEQ):
        to = (z * inner + relative(p, j // SEQ, bits), (core + j) % SEQ)
        pl.semaphore_signal(barrier, inc=1, device_id=to, device_id_type=MESH)

    @pl.when(z > 0)
    def _():
        pl.semaphore_signal(barrier, inc=1, device_id=(me - inner, core), device_id_type=MESH)

    @pl.when(z < planes - 1)
    def _():
        pl.semaphore_signal(barrier, inc=1, device_id=(me + inner, core), device_id_type=MESH)

    near = inner * SEQ - 1 + jnp.where(z > 0, 1, 0) + jnp.where(z < planes - 1, 1, 0)
    pl.semaphore_wait(barrier, near)

    swaps = []
    for i, (source, target, cols) in enumerate(
        ((k_hbm, kb, key_cols), (q_hbm, qb, heads_cols), (grad_hbm, gb, heads_cols))
    ):
        swaps.append(
            pltpu.make_async_remote_copy(
                src_ref=source.at[:, pl.ds(pl.multiple_of(other * cols, 128), cols)],
                dst_ref=target.at[pl.ds(pl.multiple_of(core * tokens, 128), tokens), :],
                send_sem=swap_send.at[i],
                recv_sem=swap_recv.at[i],
                device_id=(me, other),
                device_id_type=MESH,
            )
        )
    for swap in swaps:
        swap.start()

    loads[0].wait()
    step = 512

    def flip(i, carry):
        at = pl.multiple_of(i * step, step)
        flipped[pl.ds(at, step), :] = act[:, pl.ds(at, step)].astype(jnp.float32).T
        return carry

    lax.fori_loop(0, width // step, flip, 0)
    loads[1].wait()

    def pick(first_row):
        def some(i, carry):
            first = pl.multiple_of(i * 32, 32)
            for r in range(32):
                row = lay[first_row + first + r]
                picked[pl.ds(first + r, 1), :] = flipped[pl.ds(row, 1), :]
            return carry

        lax.fori_loop(0, rows // 32, some, 0)

    def block(k, j):
        to_p, to_core = relative(p, j // SEQ, bits), (core + j) % SEQ
        owner = turn(z, k, planes)
        return pltpu.make_async_remote_copy(
            src_ref=send.at[k, j],
            dst_ref=held.at[owner, :, pl.ds(pl.multiple_of(place * tokens, 128), tokens)],
            send_sem=a2a_send.at[k, j],
            recv_sem=a2a_recv.at[k, j],
            device_id=(z * inner + to_p, to_core),
            device_id_type=MESH,
        )

    def gather_step(k):
        owner = turn(z, k, planes)

        def to(j, carry):
            to_p, to_core = relative(p, j // SEQ, bits), (core + j) % SEQ
            pick(((owner * inner + to_p) * SEQ + to_core) * rows)
            send[k, j] = picked[...].astype(jnp.bfloat16)
            block(k, j).start()
            return carry

        lax.fori_loop(1, inner * SEQ, to, 0)
        pick(((owner * inner + p) * SEQ + core) * rows)
        held[owner, :, pl.ds(pl.multiple_of(place * tokens, 128), tokens)] = picked[...].astype(jnp.bfloat16)

    gather_step(0)

    for load in loads[2:]:
        load.wait()
    for swap in swaps:
        swap.wait_recv()
    scale = math.log2(math.e) / float(HD) ** 0.5
    key_at = lax.broadcasted_iota(jnp.int32, (tokens, 2 * tokens), 0)
    query_at = lax.broadcasted_iota(jnp.int32, (tokens, 2 * tokens), 1) % tokens
    allowed = key_at <= query_at

    def weights_of(scores):
        powers = jnp.exp2((scores - jnp.max(scores, axis=0, keepdims=True)) * scale)
        return (powers * (1.0 / jnp.sum(powers, axis=0, keepdims=True))).astype(jnp.bfloat16)

    def stacked(ref, row, col):
        return jnp.concatenate(
            [
                ref[row : row + tokens, pl.ds(pl.multiple_of(col, 128), HD)],
                ref[row : row + tokens, pl.ds(pl.multiple_of(col + HD, 128), HD)],
            ],
            axis=0,
        )

    def attend(g):
        keys = kb[:, pl.ds(pl.multiple_of(g * HD, 128), HD)]
        early = jnp.zeros((tokens, HD), jnp.float32)
        both = jnp.zeros((length, HD), jnp.float32)
        for pair in range(per_group // 2):
            col = (g * per_group + 2 * pair) * HD
            against = (((1,), (1,)), ((), ()))
            first = lax.dot_general(
                keys[:tokens], stacked(qb, 0, col), against, preferred_element_type=jnp.float32
            )
            second = lax.dot_general(
                keys, stacked(qb, tokens, col), against, preferred_element_type=jnp.float32
            )
            first = jnp.where(allowed, first, -jnp.inf)
            second = jnp.concatenate(
                [second[:tokens], jnp.where(allowed, second[tokens:], -jnp.inf)], axis=0
            )
            early += jnp.dot(
                weights_of(first), stacked(gb, 0, col), preferred_element_type=jnp.float32
            )
            both += jnp.dot(
                weights_of(second), stacked(gb, tokens, col), preferred_element_type=jnp.float32
            )
        done = jnp.concatenate([both[:tokens] + early, both[tokens:]], axis=0)
        vg[
            pl.ds(pl.multiple_of(p * length, 128), length),
            pl.ds(pl.multiple_of(core * key_cols + g * HD, 128), HD),
        ] = done.astype(jnp.bfloat16)

    def grads(from_p, from_core, c):
        return vg.at[
            pl.ds(pl.multiple_of(from_p * length, 128), length),
            pl.ds(pl.multiple_of(from_core * key_cols + c * CHUNK, 128), CHUNK),
        ]

    def gather_copy(c, jp):
        return pltpu.make_async_remote_copy(
            src_ref=grads(p, core, c), dst_ref=grads(p, core, c),
            send_sem=ag_send.at[c, jp], recv_sem=ag_recv.at[c, jp],
            device_id=(z * inner + relative(p, jp, bits), core), device_id_type=MESH,
        )

    def forward_copy(c, jp):
        from_p = relative(p, jp, bits)
        return pltpu.make_async_remote_copy(
            src_ref=grads(from_p, core, c), dst_ref=grads(from_p, core, c),
            send_sem=fwd_send.at[c, jp], recv_sem=fwd_recv.at[c, jp],
            device_id=(me, other), device_id_type=MESH,
        )

    per_chunk = CHUNK // HD
    for c in range(chunks_core):
        lax.fori_loop(c * per_chunk, (c + 1) * per_chunk, lambda g, carry: (attend(g), carry)[1], 0)
        for jp in range(1, inner):
            gather_copy(c, jp).start()
        forward_copy(c, 0).start()

    def pass_on(c):
        for jp in range(1, inner):
            gather_copy(c, jp).wait_recv()
            forward_copy(c, jp).start()

    def arrived(c):
        for jp in range(inner):
            forward_copy(c, jp).wait_recv()

    def slot(ref, owner, q):
        return ref.at[owner, :, pl.ds(pl.multiple_of(q * CHUNK, 128), CHUNK)]

    def up_copy(owner, q):
        return pltpu.make_async_remote_copy(
            src_ref=slot(part, owner, q), dst_ref=slot(up_in, owner, q),
            send_sem=rs_send.at[owner, q], recv_sem=up_sem.at[owner, q],
            device_id=(me + inner, core), device_id_type=MESH,
        )

    def down_copy(owner, q):
        return pltpu.make_async_remote_copy(
            src_ref=slot(part, owner, q), dst_ref=slot(down_in, owner, q),
            send_sem=rs_send.at[owner, q], recv_sem=down_sem.at[owner, q],
            device_id=(me - inner, core), device_id_type=MESH,
        )

    def reduce_step(k, i):
        owner = turn(z, k, planes)
        q = i % SEQ * chunks_core + i // SEQ
        cols = pl.ds(pl.multiple_of(q * CHUNK, 128), CHUNK)
        acc[...] = jnp.dot(held[owner], vg[:, cols], preferred_element_type=jnp.float32)

        @pl.when((owner >= z) & (z > 0))
        def _():
            up_copy(owner, q).wait_recv()
            acc[...] += up_in[owner, :, cols].astype(jnp.float32)

        @pl.when((owner <= z) & (z < planes - 1))
        def _():
            down_copy(owner, q).wait_recv()
            acc[...] += down_in[owner, :, cols].astype(jnp.float32)

        @pl.when(owner == z)
        def _():
            out_ref[:, cols] = acc[...]

        @pl.when(owner != z)
        def _():
            part[owner, :, cols] = acc[...].astype(jnp.bfloat16)

        @pl.when(owner > z)
        def _():
            up_copy(owner, q).start()

        @pl.when(owner < z)
        def _():
            down_copy(owner, q).start()

    def reduce_steps(k, first, last):
        lax.fori_loop(first, last, lambda i, carry: (reduce_step(k, i), carry)[1], 0)

    def took(k):
        lax.fori_loop(1, inner * SEQ, lambda j, carry: (block(k, j).wait_recv(), carry)[1], 0)

    lax.fori_loop(1, planes - 1, lambda k, carry: (gather_step(k), carry)[1], 0)
    took(0)
    for c in range(chunks_core):
        pass_on(c)
        arrived(c)
        reduce_steps(0, c * SEQ, (c + 1) * SEQ)
        if c == 0:
            gather_step(planes - 1)

    def rest(k, carry):
        took(k)
        reduce_steps(k, 0, chunks)
        return carry

    lax.fori_loop(1, planes, rest, 0)

    for swap in swaps:
        swap.wait_send()

    def left(k, carry):
        lax.fori_loop(1, inner * SEQ, lambda j, inside: (block(k, j).wait_send(), inside)[1], 0)
        return carry

    lax.fori_loop(0, planes, left, 0)
    for c in range(chunks_core):
        for jp in range(inner):
            if jp:
                gather_copy(c, jp).wait_send()
            forward_copy(c, jp).wait_send()

    def sent(k, carry):
        owner = turn(z, k, planes)
        lax.fori_loop(0, chunks, lambda q, inside: (up_copy(owner, q).wait_send(), inside)[1], 0)
        return carry

    lax.fori_loop(0, planes - 1, sent, 0)


def body(activations, queries, keys, out_grad, layout):
    members = lax.axis_size("dp")
    tokens, width = activations.shape
    inner = 1 << ((members.bit_length() - 1) // 2)
    planes = members // inner
    rows = layout.shape[0] // (members * SEQ)
    kv_width = keys.shape[1]
    chunks_core = kv_width // SEQ // CHUNK
    chunks = SEQ * chunks_core
    length = SEQ * tokens
    anywhere = pl.BlockSpec(memory_space=pl.ANY)
    dma = pltpu.SemaphoreType.DMA
    return pl.pallas_call(
        functools.partial(fused_kernel, planes=planes, inner=inner),
        out_shape=jax.ShapeDtypeStruct((rows, kv_width), jnp.float32),
        in_specs=[anywhere] * 5,
        out_specs=pl.BlockSpec(memory_space=pltpu.VMEM),
        scratch_shapes=[
            pltpu.VMEM((tokens, width), jnp.bfloat16),
            pltpu.VMEM((width, tokens), jnp.float32),
            pltpu.VMEM((rows, tokens), jnp.float32),
            pltpu.SMEM(layout.shape, jnp.int32),
            pltpu.VMEM((length, queries.shape[1] // SEQ), jnp.bfloat16),
            pltpu.VMEM((length, kv_width // SEQ), jnp.bfloat16),
            pltpu.VMEM((length, queries.shape[1] // SEQ), jnp.bfloat16),
            pltpu.VMEM((planes, inner * SEQ, rows, tokens), jnp.bfloat16),
            pltpu.VMEM((planes, rows, inner * length), jnp.bfloat16),
            pltpu.VMEM((inner * length, kv_width), jnp.bfloat16),
            pltpu.VMEM((planes, rows, kv_width), jnp.bfloat16),
            pltpu.VMEM((planes, rows, kv_width), jnp.bfloat16),
            pltpu.VMEM((planes, rows, kv_width), jnp.bfloat16),
            pltpu.VMEM((rows, CHUNK), jnp.float32),
            dma((5,)),
            dma((3,)),
            dma((3,)),
            dma((planes, inner * SEQ)),
            dma((planes, inner * SEQ)),
            dma((chunks_core, inner)),
            dma((chunks_core, inner)),
            dma((chunks_core, inner)),
            dma((chunks_core, inner)),
            dma((planes, chunks)),
            dma((planes, chunks)),
            dma((planes, chunks)),
        ],
        compiler_params=pltpu.CompilerParams(
            collective_id=0, has_side_effects=True, vmem_limit_bytes=56 * 2**20
        ),
    )(activations, queries, keys, out_grad, layout)


def solution(mesh):
    whole = ("dp", "seq")
    return jax.shard_map(
        body,
        mesh=mesh,
        in_specs=(P(whole, None),) * 4 + (P(),),
        out_specs=P(whole, None),
        check_vma=False,
    )
```

```python
import functools
import math

import jax
import jax.numpy as jnp
from jax import lax
from jax.experimental import pallas as pl
from jax.experimental.pallas import tpu as pltpu
from jax.sharding import PartitionSpec as P

H = 64
KVH = 8
HD = 128
SEQ = 2
MESH = pl.DeviceIdType.MESH


def relative(place, step, bits):
    total = 0
    for b in range(bits):
        total = total + (place // (1 << b) + step // (1 << b)) % 2 * (1 << b)
    return total


def turn(z, k, count):
    above = count - 1 - z
    sign = jnp.where(above >= z, 1, -1)
    big, small = jnp.maximum(above, z), jnp.minimum(above, z)
    later = k - (big - small)
    lone = later < 0
    distance = jnp.where(lone, big - k, small - later // 2)
    side = jnp.where(lone | (later % 2 == 1), sign, -sign)
    return z + side * distance


def fused_kernel(
    act_hbm, q_hbm, k_hbm, grad_hbm, layout_hbm, out_ref,
    act, flipped, picked, lay, qb, kb, gb, send, held, vg, down_in, up_in, part, acc,
    act_sem, lay_sem, load_sem, swap_send, swap_recv, a2a_send, a2a_recv, ag_send, ag_recv,
    fwd_send, fwd_recv, rs_send, line_sem, *, planes, inner,
):
    tokens, width = act_hbm.shape
    rows = out_ref.shape[0]
    bits = inner.bit_length() - 1
    me, core = lax.axis_index("dp"), lax.axis_index("seq")
    z, p = me // inner, me % inner
    other = 1 - core
    heads_cols, key_cols = q_hbm.shape[1] // SEQ, k_hbm.shape[1] // SEQ
    length = SEQ * tokens
    per_group = H // KVH
    groups = key_cols // HD
    half = rows // 2
    place = p * SEQ + core
    group_cols = per_group * HD
    stretch = width // 4

    cuts = ((k_hbm, kb, key_cols, 0, key_cols),) + tuple(
        (source, target, heads_cols, first, last - first)
        for first, last in ((0, group_cols), (group_cols, heads_cols))
        for source, target in ((q_hbm, qb), (grad_hbm, gb))
    )

    early_cuts = 3

    def cut(i, of_core):
        source, target, cols, first, count = cuts[i]
        return (
            source.at[:, pl.ds(pl.multiple_of(of_core * cols + first, 128), count)],
            target.at[pl.ds(pl.multiple_of(core * tokens, 128), tokens), pl.ds(first, count)],
        )

    flips = [
        pltpu.make_async_copy(
            act_hbm.at[:, pl.ds(i * stretch, stretch)],
            act.at[:, pl.ds(i * stretch, stretch)],
            act_sem.at[i],
        )
        for i in range(width // stretch)
    ]
    lay_load = pltpu.make_async_copy(layout_hbm, lay, lay_sem)
    loads = [pltpu.make_async_copy(*cut(i, core), load_sem.at[i]) for i in range(len(cuts))]
    for load in [*flips, lay_load, *loads]:
        load.start()

    barrier = pltpu.get_barrier_semaphore()
    for j in range(1, inner * SEQ):
        to = (z * inner + relative(p, j // SEQ, bits), (core + j) % SEQ)
        pl.semaphore_signal(barrier, inc=1, device_id=to, device_id_type=MESH)

    @pl.when(z > 0)
    def _():
        pl.semaphore_signal(barrier, inc=1, device_id=(me - inner, core), device_id_type=MESH)

    @pl.when(z < planes - 1)
    def _():
        pl.semaphore_signal(barrier, inc=1, device_id=(me + inner, core), device_id_type=MESH)

    near = inner * SEQ - 1 + jnp.where(z > 0, 1, 0) + jnp.where(z < planes - 1, 1, 0)
    with jax.named_scope('barrier'):
        pl.semaphore_wait(barrier, near)

    swaps = []
    for i in range(len(cuts)):
        source, target = cut(i, other)
        swaps.append(
            pltpu.make_async_remote_copy(
                src_ref=source, dst_ref=target, send_sem=swap_send, recv_sem=swap_recv.at[int(i >= early_cuts)],
                device_id=(me, other), device_id_type=MESH,
            )
        )
    for swap in swaps:
        swap.start()

    step = 512

    def flip(i, carry):
        at = pl.multiple_of(i * step, step)
        flipped[pl.ds(at, step), :] = act[:, pl.ds(at, step)].T.astype(jnp.float32)
        return carry

    for i, load in enumerate(flips):
        with jax.named_scope("act_wait"):
            load.wait()
        with jax.named_scope("flip"):
            lax.fori_loop(i * stretch // step, (i + 1) * stretch // step, flip, 0)
    lay_load.wait()

    def wait_for(like, sem):
        pltpu.make_async_remote_copy(
            src_ref=like, dst_ref=like, send_sem=sem, recv_sem=sem,
            device_id=(me, other), device_id_type=MESH,
        ).wait_recv()

    def pick(first_row):
        def some(i, carry):
            first = pl.multiple_of(i * 32, 32)
            for r in range(32):
                row = lay[first_row + first + r]
                picked[pl.ds(first + r, 1), :] = flipped[pl.ds(row, 1), :]
            return carry

        lax.fori_loop(0, half // 32, some, 0)

    def held_piece(owner, h):
        return held.at[
            owner,
            pl.ds(pl.multiple_of(h * half, 16), half),
            pl.ds(pl.multiple_of(place * tokens, 128), tokens),
        ]

    def block(k, h, j):
        to_p, to_core = relative(p, j // SEQ, bits), (core + j) % SEQ
        return pltpu.make_async_remote_copy(
            src_ref=send.at[k, j, pl.ds(pl.multiple_of(h * half, 16), half)],
            dst_ref=held_piece(turn(z, k, planes), h),
            send_sem=a2a_send,
            recv_sem=a2a_recv.at[k, h],
            device_id=(z * inner + to_p, to_core),
            device_id_type=MESH,
        )

    def gather(k, h):
        owner = turn(z, k, planes)

        def first_row(to_p, to_core):
            return ((owner * inner + to_p) * SEQ + to_core) * rows + h * half

        def to(j, carry):
            pick(first_row(relative(p, j // SEQ, bits), (core + j) % SEQ))
            send[k, j, pl.ds(pl.multiple_of(h * half, 16), half)] = picked[...].astype(jnp.bfloat16)
            block(k, h, j).start()
            return carry

        lax.fori_loop(1, inner * SEQ, to, 0)
        pick(first_row(p, core))
        held_piece(owner, h)[...] = picked[...].astype(jnp.bfloat16)

    def took(k, h):
        wait_for(send.at[0, 1:, :half], a2a_recv.at[k, h])

    scale = math.log2(math.e) / float(HD) ** 0.5
    key_at = lax.broadcasted_iota(jnp.int32, (tokens, 2 * tokens), 0)
    query_at = lax.broadcasted_iota(jnp.int32, (tokens, 2 * tokens), 1) % tokens
    allowed = key_at <= query_at

    def weights_of(scores):
        powers = jnp.exp2((scores - jnp.max(scores, axis=0, keepdims=True)) * scale)
        return (powers * (1.0 / jnp.sum(powers, axis=0, keepdims=True))).astype(jnp.bfloat16)

    def stacked(ref, row, col):
        return jnp.concatenate(
            [
                ref[row : row + tokens, pl.ds(pl.multiple_of(col, 128), HD)],
                ref[row : row + tokens, pl.ds(pl.multiple_of(col + HD, 128), HD)],
            ],
            axis=0,
        )

    def grads(from_p, from_core, g):
        return vg.at[
            pl.ds(pl.multiple_of(from_p * length, 128), length),
            pl.ds(pl.multiple_of((g * SEQ + from_core) * HD, 128), HD),
        ]

    def attend(g):
        keys = kb[:, pl.ds(pl.multiple_of(g * HD, 128), HD)]
        early = jnp.zeros((tokens, HD), jnp.float32)
        both = jnp.zeros((length, HD), jnp.float32)
        for pair in range(per_group // 2):
            col = (g * per_group + 2 * pair) * HD
            against = (((1,), (1,)), ((), ()))
            first = lax.dot_general(
                keys[:tokens], stacked(qb, 0, col), against, preferred_element_type=jnp.float32
            )
            second = lax.dot_general(
                keys, stacked(qb, tokens, col), against, preferred_element_type=jnp.float32
            )
            first = jnp.where(allowed, first, -jnp.inf)
            second = jnp.concatenate(
                [second[:tokens], jnp.where(allowed, second[tokens:], -jnp.inf)], axis=0
            )
            early += jnp.dot(
                weights_of(first), stacked(gb, 0, col), preferred_element_type=jnp.float32
            )
            both += jnp.dot(
                weights_of(second), stacked(gb, tokens, col), preferred_element_type=jnp.float32
            )
        done = jnp.concatenate([both[:tokens] + early, both[tokens:]], axis=0)
        grads(p, core, g)[...] = done.astype(jnp.bfloat16)

    def gather_copy(g, jp):
        return pltpu.make_async_remote_copy(
            src_ref=grads(p, core, g), dst_ref=grads(p, core, g),
            send_sem=ag_send, recv_sem=ag_recv.at[g],
            device_id=(z * inner + relative(p, jp, bits), core), device_id_type=MESH,
        )

    def forward_copy(g, jp):
        piece = grads(relative(p, jp, bits), core, g)
        return pltpu.make_async_remote_copy(
            src_ref=piece, dst_ref=piece,
            send_sem=fwd_send, recv_sem=fwd_recv.at[g],
            device_id=(me, other), device_id_type=MESH,
        )

    def publish(g):
        attend(g)
        for jp in range(1, inner):
            gather_copy(g, jp).start()
        forward_copy(g, 0).start()

    def pass_on(g):
        wait_for(vg.at[: (inner - 1) * length, :HD], ag_recv.at[g])
        for jp in range(1, inner):
            forward_copy(g, jp).start()

    def arrived(g):
        wait_for(vg.at[:, :HD], fwd_recv.at[g])

    def slot(ref, owner, h, g):
        return ref.at[
            owner,
            pl.ds(pl.multiple_of(h * half, 16), half),
            pl.ds(pl.multiple_of(g * SEQ * HD, 128), SEQ * HD),
        ]

    def up_copy(owner, h, g):
        return pltpu.make_async_remote_copy(
            src_ref=slot(part, owner, h, g), dst_ref=slot(up_in, owner, h, g),
            send_sem=rs_send, recv_sem=line_sem.at[owner, h, g],
            device_id=(me + inner, core), device_id_type=MESH,
        )

    def down_copy(owner, h, g, at):
        return pltpu.make_async_remote_copy(
            src_ref=slot(part, owner, h, g), dst_ref=slot(down_in, owner, h, g),
            send_sem=rs_send, recv_sem=line_sem.at[jnp.where(owner == at, planes, owner), h, g],
            device_id=(me - inner, core), device_id_type=MESH,
        )

    def reduce(k, h, g):
        owner = turn(z, k, planes)
        at_rows = pl.ds(pl.multiple_of(h * half, 16), half)
        cols = pl.ds(pl.multiple_of(g * SEQ * HD, 128), SEQ * HD)
        acc[...] = jnp.dot(held[owner, at_rows, :], vg[:, cols], preferred_element_type=jnp.float32)

        @pl.when((owner >= z) & (z > 0))
        def _():
            up_copy(owner, h, g).wait_recv()
            acc[...] += slot(up_in, owner, h, g)[...].astype(jnp.float32)

        @pl.when((owner <= z) & (z < planes - 1))
        def _():
            down_copy(owner, h, g, z).wait_recv()
            acc[...] += slot(down_in, owner, h, g)[...].astype(jnp.float32)

        @pl.when(owner == z)
        def _():
            for c in range(SEQ):
                out_ref[at_rows, pl.ds(pl.multiple_of((c * groups + g) * HD, 128), HD)] = acc[
                    :, c * HD : (c + 1) * HD
                ]

        @pl.when(owner != z)
        def _():
            slot(part, owner, h, g)[...] = acc[...].astype(jnp.bfloat16)

        @pl.when(owner > z)
        def _():
            up_copy(owner, h, g).start()

        @pl.when(owner < z)
        def _():
            down_copy(owner, h, g, z - 1).start()

    def each(first, last, step):
        lax.fori_loop(first, last, lambda i, carry: (step(i), carry)[1], 0)

    with jax.named_scope("g00"):
        gather(0, 0)
    with jax.named_scope("qwait"):
        for load in loads[:early_cuts]:
            load.wait()
        wait_for(qb.at[:tokens, : 2 * group_cols + key_cols], swap_recv.at[0])
    with jax.named_scope("a0"):
        publish(0)
    with jax.named_scope("g01"):
        gather(0, 1)
    with jax.named_scope("qwait2"):
        for load in loads[early_cuts:]:
            load.wait()
        wait_for(qb.at[:, group_cols:], swap_recv.at[1])
    with jax.named_scope("a123"):
        each(1, groups, publish)
    for g in range(groups):
        with jax.named_scope(f"pass{g}"):
            pass_on(g)
        if g < 2 * (planes - 1):
            with jax.named_scope(f"ga{g}"):
                gather(1 + g // 2, g % 2)
        if g == 0:
            with jax.named_scope("took00"):
                took(0, 0)
        with jax.named_scope(f"arr{g}"):
            arrived(g)
        with jax.named_scope(f"red0_{g}"):
            reduce(0, 0, g)
            if g == 0:
                with jax.named_scope("took01"):
                    took(0, 1)
            reduce(0, 1, g)
    with jax.named_scope("glast"):
        each(groups, 2 * (planes - 1), lambda i: gather(1 + i // 2, i % 2))

    def rest(i):
        with jax.named_scope("took"):
            took(i // 2, i % 2)
        with jax.named_scope("red"):
            each(0, groups, lambda g: reduce(i // 2, i % 2, g))

    each(2, 2 * planes, rest)

    with jax.named_scope("t0"):
        for ref in (qb, gb, kb):
            wait_for(ref.at[:tokens], swap_send)
        wait_for(send.at[:, 1:], a2a_send)
        wait_for(vg.at[: (inner - 1) * length, : groups * HD], ag_send)
        wait_for(vg.at[:, : groups * HD], fwd_send)
    with jax.named_scope("t3"):
        wait_for(part.at[1:], rs_send)


def body(activations, queries, keys, out_grad, layout):
    members = lax.axis_size("dp")
    tokens, width = activations.shape
    inner = 1 << ((members.bit_length() - 1) // 2)
    planes = members // inner
    rows = layout.shape[0] // (members * SEQ)
    kv_width = keys.shape[1]
    groups = kv_width // SEQ // HD
    length = SEQ * tokens
    dma = pltpu.SemaphoreType.DMA
    operands = (activations, queries, keys, out_grad, layout)
    return pl.pallas_call(
        functools.partial(fused_kernel, planes=planes, inner=inner),
        out_shape=jax.ShapeDtypeStruct((rows, kv_width), jnp.float32),
        in_specs=[pl.BlockSpec(memory_space=pltpu.HBM)] * len(operands),
        out_specs=pl.BlockSpec(memory_space=pltpu.VMEM),
        scratch_shapes=[
            pltpu.VMEM((tokens, width), jnp.bfloat16),
            pltpu.VMEM((width, tokens), jnp.float32),
            pltpu.VMEM((rows // 2, tokens), jnp.float32),
            pltpu.SMEM(layout.shape, jnp.int32),
            pltpu.VMEM((length, queries.shape[1] // SEQ), jnp.bfloat16),
            pltpu.VMEM((length, kv_width // SEQ), jnp.bfloat16),
            pltpu.VMEM((length, queries.shape[1] // SEQ), jnp.bfloat16),
            pltpu.VMEM((planes, inner * SEQ, rows, tokens), jnp.bfloat16),
            pltpu.VMEM((planes, rows, inner * length), jnp.bfloat16),
            pltpu.VMEM((inner * length, kv_width), jnp.bfloat16),
            pltpu.VMEM((planes, rows, kv_width), jnp.bfloat16),
            pltpu.VMEM((planes, rows, kv_width), jnp.bfloat16),
            pltpu.VMEM((planes, rows, kv_width), jnp.bfloat16),
            pltpu.VMEM((rows // 2, SEQ * HD), jnp.float32),
            dma((4,)),
            dma(()),
            dma((5,)),
            dma(()),
            dma((2,)),
            dma(()),
            dma((planes, 2)),
            dma(()),
            dma((groups,)),
            dma(()),
            dma((groups,)),
            dma(()),
            dma((planes + 1, 2, groups)),
        ],
        compiler_params=pltpu.CompilerParams(
            collective_id=0, has_side_effects=True, vmem_limit_bytes=32 * 2**20
        ),
    )(*(pltpu.with_memory_space_constraint(x, pltpu.HBM) for x in operands))


def solution(mesh):
    whole = ("dp", "seq")
    return jax.shard_map(
        body,
        mesh=mesh,
        in_specs=(P(whole, None),) * 4 + (P(),),
        out_specs=P(whole, None),
        check_vma=False,
    )
```

```python
import functools
import math

import jax
import jax.numpy as jnp
from jax import lax
from jax.experimental import pallas as pl
from jax.experimental.pallas import tpu as pltpu
from jax.sharding import PartitionSpec as P

H = 64
KVH = 8
HD = 128
SEQ = 2
MESH = pl.DeviceIdType.MESH


def relative(place, step, bits):
    total = 0
    for b in range(bits):
        total = total + (place // (1 << b) + step // (1 << b)) % 2 * (1 << b)
    return total


def turn(z, k, count):
    above = count - 1 - z
    sign = jnp.where(above >= z, 1, -1)
    big, small = jnp.maximum(above, z), jnp.minimum(above, z)
    later = k - (big - small)
    lone = later < 0
    distance = jnp.where(lone, big - k, small - later // 2)
    side = jnp.where(lone | (later % 2 == 1), sign, -sign)
    return z + side * distance


def fused_kernel(
    act_hbm, q_hbm, k_hbm, grad_hbm, layout_hbm, out_ref,
    act, flipped, picked, lay, qb, kb, gb, send, held, vg, down_in, up_in, part, acc,
    act_sem, lay_sem, load_sem, swap_send, swap_recv, a2a_send, a2a_recv, ag_send, ag_recv,
    fwd_send, fwd_recv, rs_send, line_sem, end_sem, *, planes, inner,
):
    tokens, width = act_hbm.shape
    rows = out_ref.shape[0]
    bits = inner.bit_length() - 1
    me, core = lax.axis_index("dp"), lax.axis_index("seq")
    z, p = me // inner, me % inner
    other = 1 - core
    heads_cols, key_cols = q_hbm.shape[1] // SEQ, k_hbm.shape[1] // SEQ
    length = SEQ * tokens
    per_group = H // KVH
    groups = key_cols // HD
    half = rows // 2
    place = p * SEQ + core
    group_cols = per_group * HD
    stretch = width // 4

    cuts = ((k_hbm, kb, key_cols, 0, key_cols),) + tuple(
        (source, target, heads_cols, first, last - first)
        for first, last in ((0, group_cols), (group_cols, heads_cols))
        for source, target in ((q_hbm, qb), (grad_hbm, gb))
    )

    early_cuts = 3

    def cut(i, of_core):
        source, target, cols, first, count = cuts[i]
        return (
            source.at[:, pl.ds(pl.multiple_of(of_core * cols + first, 128), count)],
            target.at[pl.ds(pl.multiple_of(core * tokens, 128), tokens), pl.ds(first, count)],
        )

    flips = [
        pltpu.make_async_copy(
            act_hbm.at[:, pl.ds(i * stretch, stretch)],
            act.at[:, pl.ds(i * stretch, stretch)],
            act_sem.at[i],
        )
        for i in range(width // stretch)
    ]
    lay_load = pltpu.make_async_copy(layout_hbm, lay, lay_sem)
    loads = [pltpu.make_async_copy(*cut(i, core), load_sem.at[i]) for i in range(len(cuts))]
    for load in [*flips, lay_load]:
        load.start()

    barrier = pltpu.get_barrier_semaphore()
    for j in range(1, inner * SEQ):
        to = (z * inner + relative(p, j // SEQ, bits), (core + j) % SEQ)
        pl.semaphore_signal(barrier, inc=1, device_id=to, device_id_type=MESH)

    @pl.when(z > 0)
    def _():
        pl.semaphore_signal(barrier, inc=1, device_id=(me - inner, core), device_id_type=MESH)

    @pl.when(z < planes - 1)
    def _():
        pl.semaphore_signal(barrier, inc=1, device_id=(me + inner, core), device_id_type=MESH)

    near = inner * SEQ - 1 + jnp.where(z > 0, 1, 0) + jnp.where(z < planes - 1, 1, 0)

    swaps = []
    for i in range(len(cuts)):
        source, target = cut(i, other)
        swaps.append(
            pltpu.make_async_remote_copy(
                src_ref=source, dst_ref=target, send_sem=swap_send, recv_sem=swap_recv.at[int(i >= early_cuts)],
                device_id=(me, other), device_id_type=MESH,
            )
        )
    step = 1024

    def flip(i, carry):
        at = pl.multiple_of(i * step, step)
        flipped[pl.ds(at, step), :] = act[:, pl.ds(at, step)].T.astype(jnp.float32)
        return carry

    for i, load in enumerate(flips):
        with jax.named_scope("act_wait"):
            load.wait()
        if i == 0:
            for other_load in loads:
                other_load.start()
        with jax.named_scope("flip"):
            lax.fori_loop(i * stretch // step, (i + 1) * stretch // step, flip, 0)
        if i == 1:
            with jax.named_scope("barrier"):
                pl.semaphore_wait(barrier, near)
            for swap in swaps:
                swap.start()
    lay_load.wait()

    def wait_for(like, sem):
        pltpu.make_async_remote_copy(
            src_ref=like, dst_ref=like, send_sem=sem, recv_sem=sem,
            device_id=(me, other), device_id_type=MESH,
        ).wait_recv()

    def pick(first_row):
        def some(i, carry):
            first = pl.multiple_of(i * 32, 32)
            for r in range(32):
                row = lay[first_row + first + r]
                picked[pl.ds(first + r, 1), :] = flipped[pl.ds(row, 1), :]
            return carry

        lax.fori_loop(0, half // 32, some, 0)

    def held_piece(owner, h):
        return held.at[
            owner,
            pl.ds(pl.multiple_of(h * half, 16), half),
            pl.ds(pl.multiple_of(place * tokens, 128), tokens),
        ]

    def block(k, h, j):
        to_p, to_core = relative(p, j // SEQ, bits), (core + j) % SEQ
        return pltpu.make_async_remote_copy(
            src_ref=send.at[k, j, pl.ds(pl.multiple_of(h * half, 16), half)],
            dst_ref=held_piece(turn(z, k, planes), h),
            send_sem=a2a_send,
            recv_sem=a2a_recv.at[k, h],
            device_id=(z * inner + to_p, to_core),
            device_id_type=MESH,
        )

    def gather(k, h):
        owner = turn(z, k, planes)

        def first_row(to_p, to_core):
            return ((owner * inner + to_p) * SEQ + to_core) * rows + h * half

        def to(j, carry):
            pick(first_row(relative(p, j // SEQ, bits), (core + j) % SEQ))
            send[k, j, pl.ds(pl.multiple_of(h * half, 16), half)] = picked[...].astype(jnp.bfloat16)
            block(k, h, j).start()
            return carry

        lax.fori_loop(1, inner * SEQ, to, 0)
        pick(first_row(p, core))
        held_piece(owner, h)[...] = picked[...].astype(jnp.bfloat16)

    def took(k, h):
        wait_for(send.at[0, 1:, :half], a2a_recv.at[k, h])

    scale = math.log2(math.e) / float(HD) ** 0.5
    key_at = lax.broadcasted_iota(jnp.int32, (tokens, 2 * tokens), 0)
    query_at = lax.broadcasted_iota(jnp.int32, (tokens, 2 * tokens), 1) % tokens
    allowed = key_at <= query_at

    def weights_of(scores):
        powers = jnp.exp2((scores - jnp.max(scores, axis=0, keepdims=True)) * scale)
        return (powers * (1.0 / jnp.sum(powers, axis=0, keepdims=True))).astype(jnp.bfloat16)

    def stacked(ref, row, col):
        return jnp.concatenate(
            [
                ref[row : row + tokens, pl.ds(pl.multiple_of(col, 128), HD)],
                ref[row : row + tokens, pl.ds(pl.multiple_of(col + HD, 128), HD)],
            ],
            axis=0,
        )

    def grads(from_p, at):
        return vg.at[
            pl.ds(pl.multiple_of(from_p * length, 128), length),
            pl.ds(pl.multiple_of(at * HD, 128), HD),
        ]

    def attend(g):
        keys = kb[:, pl.ds(pl.multiple_of(g * HD, 128), HD)]
        early = jnp.zeros((tokens, HD), jnp.float32)
        both = jnp.zeros((length, HD), jnp.float32)
        for pair in range(per_group // 2):
            col = (g * per_group + 2 * pair) * HD
            against = (((1,), (1,)), ((), ()))
            first = lax.dot_general(
                keys[:tokens], stacked(qb, 0, col), against, preferred_element_type=jnp.float32
            )
            second = lax.dot_general(
                keys, stacked(qb, tokens, col), against, preferred_element_type=jnp.float32
            )
            first = jnp.where(allowed, first, -jnp.inf)
            second = jnp.concatenate(
                [second[:tokens], jnp.where(allowed, second[tokens:], -jnp.inf)], axis=0
            )
            early += jnp.dot(
                weights_of(first), stacked(gb, 0, col), preferred_element_type=jnp.float32
            )
            both += jnp.dot(
                weights_of(second), stacked(gb, tokens, col), preferred_element_type=jnp.float32
            )
        done = jnp.concatenate([both[:tokens] + early, both[tokens:]], axis=0)
        grads(p, 2 * g)[...] = done.astype(jnp.bfloat16)

    def gather_copy(g, jp):
        return pltpu.make_async_remote_copy(
            src_ref=grads(p, 2 * g), dst_ref=grads(p, 2 * g),
            send_sem=ag_send, recv_sem=ag_recv.at[g],
            device_id=(z * inner + relative(p, jp, bits), core), device_id_type=MESH,
        )

    def forward_copy(g, jp):
        from_p = relative(p, jp, bits)
        return pltpu.make_async_remote_copy(
            src_ref=grads(from_p, 2 * g), dst_ref=grads(from_p, 2 * g + 1),
            send_sem=fwd_send, recv_sem=fwd_recv.at[g],
            device_id=(me, other), device_id_type=MESH,
        )

    def publish(g):
        attend(g)
        for jp in range(1, inner):
            gather_copy(g, jp).start()
        forward_copy(g, 0).start()

    def pass_on(g):
        wait_for(vg.at[: (inner - 1) * length, :HD], ag_recv.at[g])
        for jp in range(1, inner):
            forward_copy(g, jp).start()

    def arrived(g):
        wait_for(vg.at[:, :HD], fwd_recv.at[g])

    def slot(ref, owner, h, at, wide):
        return ref.at[
            owner,
            pl.ds(pl.multiple_of(h * half, 16), half),
            pl.ds(pl.multiple_of(at * HD, 128), wide * HD),
        ]

    def up_copy(owner, h, at, wide):
        sem = end_sem.at[1, h, at] if wide == 1 else line_sem.at[owner - 1, h, at // 2]
        return pltpu.make_async_remote_copy(
            src_ref=slot(part, owner, h, at, wide), dst_ref=slot(up_in, owner, h, at, wide),
            send_sem=rs_send, recv_sem=sem,
            device_id=(me + inner, core), device_id_type=MESH,
        )

    def down_copy(owner, h, at, wide, to):
        if wide == 1:
            sem = end_sem.at[0, h, at]
        else:
            sem = line_sem.at[jnp.where(owner == to, planes, owner) - 1 - jnp.where(owner == to, 1, 0), h, at // 2]
        return pltpu.make_async_remote_copy(
            src_ref=slot(part, owner, h, at, wide), dst_ref=slot(down_in, owner, h, at, wide),
            send_sem=rs_send, recv_sem=sem,
            device_id=(me - inner, core), device_id_type=MESH,
        )

    def reduce(k, h, at, wide):
        owner = turn(z, k, planes)
        at_rows = pl.ds(pl.multiple_of(h * half, 16), half)
        cols = pl.ds(pl.multiple_of(at * HD, 128), wide * HD)
        here = acc.at[:, : wide * HD]
        here[...] = jnp.dot(held[owner, at_rows, :], vg[:, cols], preferred_element_type=jnp.float32)

        @pl.when((owner >= z) & (z > 0))
        def _():
            up_copy(owner, h, at, wide).wait_recv()
            here[...] += slot(up_in, owner, h, at, wide)[...].astype(jnp.float32)

        @pl.when((owner <= z) & (z < planes - 1))
        def _():
            down_copy(owner, h, at, wide, z).wait_recv()
            here[...] += slot(down_in, owner, h, at, wide)[...].astype(jnp.float32)

        @pl.when(owner == z)
        def _():
            for c in range(wide):
                of_core = (core + at + c) % SEQ
                out_ref[at_rows, pl.ds(pl.multiple_of((of_core * groups + (at + c) // 2) * HD, 128), HD)] = acc[
                    :, c * HD : (c + 1) * HD
                ]

        @pl.when(owner != z)
        def _():
            slot(part, owner, h, at, wide)[...] = here[...].astype(jnp.bfloat16)

        @pl.when(owner > z)
        def _():
            up_copy(owner, h, at, wide).start()

        @pl.when(owner < z)
        def _():
            down_copy(owner, h, at, wide, z - 1).start()

    def reduce_all(k, h):
        owner = turn(z, k, planes)
        at_end = (owner == 0) | (owner == planes - 1)

        @pl.when(at_end)
        def _():
            each(0, 2 * groups, lambda at: reduce(k, h, at, 1))

        @pl.when(jnp.logical_not(at_end))
        def _():
            each(0, groups, lambda g: reduce(k, h, 2 * g, 2))

    def each(first, last, step):
        lax.fori_loop(first, last, lambda i, carry: (step(i), carry)[1], 0)

    with jax.named_scope("g00"):
        gather(0, 0)
    with jax.named_scope("qwait"):
        for load in loads[:early_cuts]:
            load.wait()
        wait_for(qb.at[:tokens, : 2 * group_cols + key_cols], swap_recv.at[0])
    with jax.named_scope("a0"):
        publish(0)
    with jax.named_scope("g01"):
        gather(0, 1)
    with jax.named_scope("qwait2"):
        for load in loads[early_cuts:]:
            load.wait()
        wait_for(qb.at[:, group_cols:], swap_recv.at[1])
    with jax.named_scope("a123"):
        each(1, groups, publish)
    later = [lambda i=i: gather(i // 2, i % 2) for i in range(2, 2 * planes)]

    def next_gather():
        if later:
            with jax.named_scope("gnext"):
                later.pop(0)()

    next_gather()
    for g in range(groups):
        with jax.named_scope(f"pass{g}"):
            pass_on(g)
        if g == 0:
            with jax.named_scope("took00"):
                took(0, 0)
        with jax.named_scope(f"red0_{g}own"):
            reduce(0, 0, 2 * g, 1)
            if g:
                reduce(0, 1, 2 * g, 1)
        if g == 0:
            next_gather()
        with jax.named_scope(f"arr{g}"):
            arrived(g)
        with jax.named_scope(f"red0_{g}other"):
            reduce(0, 0, 2 * g + 1, 1)
            if g == 0:
                with jax.named_scope("took01"):
                    took(0, 1)
                reduce(0, 1, 0, 1)
            reduce(0, 1, 2 * g + 1, 1)
        if g == 0:
            next_gather()
        if g < groups - 1:
            next_gather()

    def rest(i):
        with jax.named_scope("took"):
            took(i // 2, i % 2)
        with jax.named_scope("red"):
            reduce_all(i // 2, i % 2)

    rest(2)
    with jax.named_scope("glast"):
        each(2 * planes - len(later), 2 * planes, lambda i: gather(i // 2, i % 2))
    each(3, 2 * planes, rest)

    with jax.named_scope("t0"):
        for ref in (qb, gb, kb):
            wait_for(ref.at[:tokens], swap_send)
        wait_for(send.at[:, 1:], a2a_send)
        wait_for(vg.at[: (inner - 1) * length, : groups * HD], ag_send)
        wait_for(vg.at[:, : groups * HD], fwd_send)
    with jax.named_scope("t3"):
        wait_for(part.at[1:], rs_send)


def body(activations, queries, keys, out_grad, layout):
    members = lax.axis_size("dp")
    tokens, width = activations.shape
    inner = 1 << ((members.bit_length() - 1) // 2)
    planes = members // inner
    rows = layout.shape[0] // (members * SEQ)
    kv_width = keys.shape[1]
    groups = kv_width // SEQ // HD
    length = SEQ * tokens
    dma = pltpu.SemaphoreType.DMA
    operands = (activations, queries, keys, out_grad, layout)
    return pl.pallas_call(
        functools.partial(fused_kernel, planes=planes, inner=inner),
        out_shape=jax.ShapeDtypeStruct((rows, kv_width), jnp.float32),
        in_specs=[pl.BlockSpec(memory_space=pltpu.HBM)] * len(operands),
        out_specs=pl.BlockSpec(memory_space=pltpu.VMEM),
        scratch_shapes=[
            pltpu.VMEM((tokens, width), jnp.bfloat16),
            pltpu.VMEM((width, tokens), jnp.float32),
            pltpu.VMEM((rows // 2, tokens), jnp.float32),
            pltpu.SMEM(layout.shape, jnp.int32),
            pltpu.VMEM((length, queries.shape[1] // SEQ), jnp.bfloat16),
            pltpu.VMEM((length, kv_width // SEQ), jnp.bfloat16),
            pltpu.VMEM((length, queries.shape[1] // SEQ), jnp.bfloat16),
            pltpu.VMEM((planes, inner * SEQ, rows, tokens), jnp.bfloat16),
            pltpu.VMEM((planes, rows, inner * length), jnp.bfloat16),
            pltpu.VMEM((inner * length, kv_width), jnp.bfloat16),
            pltpu.VMEM((planes, rows, kv_width), jnp.bfloat16),
            pltpu.VMEM((planes, rows, kv_width), jnp.bfloat16),
            pltpu.VMEM((planes, rows, kv_width), jnp.bfloat16),
            pltpu.VMEM((rows // 2, SEQ * HD), jnp.float32),
            dma((4,)),
            dma(()),
            dma((5,)),
            dma(()),
            dma((2,)),
            dma(()),
            dma((planes, 2)),
            dma(()),
            dma((groups,)),
            dma(()),
            dma((groups,)),
            dma(()),
            dma((planes - 1, 2, groups)),
            dma((2, 2, 2 * groups)),
        ],
        compiler_params=pltpu.CompilerParams(
            collective_id=0, has_side_effects=True, vmem_limit_bytes=32 * 2**20
        ),
    )(*(pltpu.with_memory_space_constraint(x, pltpu.HBM) for x in operands))


def solution(mesh):
    whole = ("dp", "seq")
    return jax.shard_map(
        body,
        mesh=mesh,
        in_specs=(P(whole, None),) * 4 + (P(),),
        out_specs=P(whole, None),
        check_vma=False,
    )
```

```python
import functools
import math

import jax
import jax.numpy as jnp
from jax import lax
from jax.experimental import pallas as pl
from jax.experimental.pallas import tpu as pltpu
from jax.sharding import PartitionSpec as P

H = 64
KVH = 8
HD = 128
SEQ = 2
MESH = pl.DeviceIdType.MESH


def relative(place, step, bits):
    total = 0
    for b in range(bits):
        total = total + (place // (1 << b) + step // (1 << b)) % 2 * (1 << b)
    return total


def turn(z, k, count):
    above = count - 1 - z
    sign = jnp.where(above >= z, 1, -1)
    big, small = jnp.maximum(above, z), jnp.minimum(above, z)
    later = k - (big - small)
    lone = later < 0
    distance = jnp.where(lone, big - k, small - later // 2)
    side = jnp.where(lone | (later % 2 == 1), sign, -sign)
    return z + side * distance


def fused_kernel(
    act_hbm, q_hbm, k_hbm, grad_hbm, layout_hbm, out_ref,
    act, flipped, picked, lay, qb, kb, gb, send, held, vg, down_in, up_in, part, acc,
    act_sem, lay_sem, load_sem, swap_send, swap_recv, a2a_send, a2a_recv, ag_send, ag_recv,
    fwd_send, fwd_recv, rs_send, line_sem, end_sem, *, planes, inner,
):
    tokens, width = act_hbm.shape
    rows = out_ref.shape[0]
    bits = inner.bit_length() - 1
    me, core = lax.axis_index("dp"), lax.axis_index("seq")
    z, p = me // inner, me % inner
    other = 1 - core
    heads_cols, key_cols = q_hbm.shape[1] // SEQ, k_hbm.shape[1] // SEQ
    length = SEQ * tokens
    per_group = H // KVH
    groups = key_cols // HD
    half = rows // 2
    place = p * SEQ + core
    group_cols = per_group * HD
    stretch = width // 4

    cuts = ((k_hbm, kb, key_cols, 0, key_cols),) + tuple(
        (source, target, heads_cols, first, last - first)
        for first, last in ((0, group_cols), (group_cols, heads_cols))
        for source, target in ((q_hbm, qb), (grad_hbm, gb))
    )

    early_cuts = 3

    def cut(i, of_core):
        source, target, cols, first, count = cuts[i]
        return (
            source.at[:, pl.ds(pl.multiple_of(of_core * cols + first, 128), count)],
            target.at[pl.ds(pl.multiple_of(core * tokens, 128), tokens), pl.ds(first, count)],
        )

    flips = [
        pltpu.make_async_copy(
            act_hbm.at[:, pl.ds(i * stretch, stretch)],
            act.at[:, pl.ds(i * stretch, stretch)],
            act_sem.at[i],
        )
        for i in range(width // stretch)
    ]
    lay_load = pltpu.make_async_copy(layout_hbm, lay, lay_sem)
    loads = [pltpu.make_async_copy(*cut(i, core), load_sem.at[int(i >= early_cuts)]) for i in range(len(cuts))]
    for load in [*flips, lay_load]:
        load.start()

    barrier = pltpu.get_barrier_semaphore()
    for j in range(1, inner * SEQ):
        to = (z * inner + relative(p, j // SEQ, bits), (core + j) % SEQ)
        pl.semaphore_signal(barrier, inc=1, device_id=to, device_id_type=MESH)

    @pl.when(z > 0)
    def _():
        pl.semaphore_signal(barrier, inc=1, device_id=(me - inner, core), device_id_type=MESH)

    @pl.when(z < planes - 1)
    def _():
        pl.semaphore_signal(barrier, inc=1, device_id=(me + inner, core), device_id_type=MESH)

    near = inner * SEQ - 1 + jnp.where(z > 0, 1, 0) + jnp.where(z < planes - 1, 1, 0)

    swaps = []
    for i in range(len(cuts)):
        source, target = cut(i, other)
        swaps.append(
            pltpu.make_async_remote_copy(
                src_ref=source, dst_ref=target, send_sem=swap_send, recv_sem=swap_recv.at[int(i >= early_cuts)],
                device_id=(me, other), device_id_type=MESH,
            )
        )
    step = 1024

    def flip(i, carry):
        at = pl.multiple_of(i * step, step)
        flipped[pl.ds(at, step), :] = act[:, pl.ds(at, step)].T.astype(jnp.float32)
        return carry

    for i, load in enumerate(flips):
        with jax.named_scope("act_wait"):
            load.wait()
        if i == 0:
            for other_load in loads:
                other_load.start()
        with jax.named_scope("flip"):
            lax.fori_loop(i * stretch // step, (i + 1) * stretch // step, flip, 0)
        if i == 1:
            with jax.named_scope("barrier"):
                pl.semaphore_wait(barrier, near)
            for swap in swaps:
                swap.start()
    lay_load.wait()

    def wait_for(like, sem):
        pltpu.make_async_remote_copy(
            src_ref=like, dst_ref=like, send_sem=sem, recv_sem=sem,
            device_id=(me, other), device_id_type=MESH,
        ).wait_recv()

    def pick(first_row):
        def some(i, carry):
            first = pl.multiple_of(i * 32, 32)
            for r in range(32):
                row = lay[first_row + first + r]
                picked[pl.ds(first + r, 1), :] = flipped[pl.ds(row, 1), :]
            return carry

        lax.fori_loop(0, half // 32, some, 0)

    def held_piece(owner, h):
        return held.at[
            owner,
            pl.ds(pl.multiple_of(h * half, 16), half),
            pl.ds(pl.multiple_of(place * tokens, 128), tokens),
        ]

    def block(k, h, j):
        to_p, to_core = relative(p, j // SEQ, bits), (core + j) % SEQ
        return pltpu.make_async_remote_copy(
            src_ref=send.at[k, j, pl.ds(pl.multiple_of(h * half, 16), half)],
            dst_ref=held_piece(turn(z, k, planes), h),
            send_sem=a2a_send,
            recv_sem=a2a_recv.at[k, h],
            device_id=(z * inner + to_p, to_core),
            device_id_type=MESH,
        )

    def gather(k, h):
        owner = turn(z, k, planes)

        def first_row(to_p, to_core):
            return ((owner * inner + to_p) * SEQ + to_core) * rows + h * half

        def to(i, carry):
            j = inner * SEQ - i
            pick(first_row(relative(p, j // SEQ, bits), (core + j) % SEQ))
            send[k, j, pl.ds(pl.multiple_of(h * half, 16), half)] = picked[...].astype(jnp.bfloat16)
            block(k, h, j).start()
            return carry

        lax.fori_loop(1, inner * SEQ, to, 0)
        pick(first_row(p, core))
        held_piece(owner, h)[...] = picked[...].astype(jnp.bfloat16)

    def took(k, h):
        wait_for(send.at[0, 1:, :half], a2a_recv.at[k, h])

    scale = math.log2(math.e) / float(HD) ** 0.5
    key_at = lax.broadcasted_iota(jnp.int32, (tokens, 2 * tokens), 0)
    query_at = lax.broadcasted_iota(jnp.int32, (tokens, 2 * tokens), 1) % tokens
    allowed = key_at <= query_at

    def weights_of(scores):
        powers = jnp.exp2((scores - jnp.max(scores, axis=0, keepdims=True)) * scale)
        return (powers * (1.0 / jnp.sum(powers, axis=0, keepdims=True))).astype(jnp.bfloat16)

    def stacked(ref, row, col):
        return jnp.concatenate(
            [
                ref[row : row + tokens, pl.ds(pl.multiple_of(col, 128), HD)],
                ref[row : row + tokens, pl.ds(pl.multiple_of(col + HD, 128), HD)],
            ],
            axis=0,
        )

    def grads(from_p, at):
        return vg.at[
            pl.ds(pl.multiple_of(from_p * length, 128), length),
            pl.ds(pl.multiple_of(at * HD, 128), HD),
        ]

    def attend(g):
        keys = kb[:, pl.ds(pl.multiple_of(g * HD, 128), HD)]
        early = jnp.zeros((tokens, HD), jnp.float32)
        both = jnp.zeros((length, HD), jnp.float32)
        for pair in range(per_group // 2):
            col = (g * per_group + 2 * pair) * HD
            against = (((1,), (1,)), ((), ()))
            first = lax.dot_general(
                keys[:tokens], stacked(qb, 0, col), against, preferred_element_type=jnp.float32
            )
            second = lax.dot_general(
                keys, stacked(qb, tokens, col), against, preferred_element_type=jnp.float32
            )
            first = jnp.where(allowed, first, -jnp.inf)
            second = jnp.concatenate(
                [second[:tokens], jnp.where(allowed, second[tokens:], -jnp.inf)], axis=0
            )
            early += jnp.dot(
                weights_of(first), stacked(gb, 0, col), preferred_element_type=jnp.float32
            )
            both += jnp.dot(
                weights_of(second), stacked(gb, tokens, col), preferred_element_type=jnp.float32
            )
        done = jnp.concatenate([both[:tokens] + early, both[tokens:]], axis=0)
        grads(p, 2 * g)[...] = done.astype(jnp.bfloat16)

    def gather_copy(g, jp):
        return pltpu.make_async_remote_copy(
            src_ref=grads(p, 2 * g), dst_ref=grads(p, 2 * g),
            send_sem=ag_send, recv_sem=ag_recv.at[g],
            device_id=(z * inner + relative(p, jp, bits), core), device_id_type=MESH,
        )

    def forward_copy(g, jp):
        from_p = relative(p, jp, bits)
        return pltpu.make_async_remote_copy(
            src_ref=grads(from_p, 2 * g), dst_ref=grads(from_p, 2 * g + 1),
            send_sem=fwd_send, recv_sem=fwd_recv.at[g],
            device_id=(me, other), device_id_type=MESH,
        )

    def publish(g):
        attend(g)
        for jp in reversed(range(1, inner)):
            gather_copy(g, jp).start()
        forward_copy(g, 0).start()

    def pass_on(g):
        wait_for(vg.at[: (inner - 1) * length, :HD], ag_recv.at[g])
        for jp in range(1, inner):
            forward_copy(g, jp).start()

    def arrived(g):
        wait_for(vg.at[:, :HD], fwd_recv.at[g])

    def slot(ref, owner, h, at, wide):
        count = rows if h is None else half
        first = 0 if h is None else pl.multiple_of(h * half, 16)
        return ref.at[owner, pl.ds(first, count), pl.ds(pl.multiple_of(at * HD, 128), wide * HD)]

    def end_sem_of(end, h, at):
        return end_sem.at[end, at if h is None or h == 0 else 2 * groups + at]

    def up_copy(owner, h, at, wide):
        sem = end_sem_of(1, h, at) if wide == 1 else line_sem.at[owner - 1, h, at // 2]
        return pltpu.make_async_remote_copy(
            src_ref=slot(part, owner, h, at, wide), dst_ref=slot(up_in, owner, h, at, wide),
            send_sem=rs_send, recv_sem=sem,
            device_id=(me + inner, core), device_id_type=MESH,
        )

    def down_copy(owner, h, at, wide, to):
        if wide == 1:
            sem = end_sem_of(0, h, at)
        else:
            sem = line_sem.at[jnp.where(owner == to, planes, owner) - 1 - jnp.where(owner == to, 1, 0), h, at // 2]
        return pltpu.make_async_remote_copy(
            src_ref=slot(part, owner, h, at, wide), dst_ref=slot(down_in, owner, h, at, wide),
            send_sem=rs_send, recv_sem=sem,
            device_id=(me - inner, core), device_id_type=MESH,
        )

    def reduce(k, h, at, wide):
        owner = turn(z, k, planes)
        count = rows if h is None else half
        at_rows = pl.ds(0 if h is None else pl.multiple_of(h * half, 16), count)
        cols = pl.ds(pl.multiple_of(at * HD, 128), wide * HD)
        here = acc.at[:count, : wide * HD]
        here[...] = jnp.dot(held[owner, at_rows, :], vg[:, cols], preferred_element_type=jnp.float32)

        @pl.when((owner >= z) & (z > 0))
        def _():
            up_copy(owner, h, at, wide).wait_recv()
            here[...] += slot(up_in, owner, h, at, wide)[...].astype(jnp.float32)

        @pl.when((owner <= z) & (z < planes - 1))
        def _():
            down_copy(owner, h, at, wide, z).wait_recv()
            here[...] += slot(down_in, owner, h, at, wide)[...].astype(jnp.float32)

        @pl.when(owner == z)
        def _():
            for c in range(wide):
                of_core = (core + at + c) % SEQ
                out_ref[at_rows, pl.ds(pl.multiple_of((of_core * groups + (at + c) // 2) * HD, 128), HD)] = acc[
                    :count, c * HD : (c + 1) * HD
                ]

        @pl.when(owner != z)
        def _():
            slot(part, owner, h, at, wide)[...] = here[...].astype(jnp.bfloat16)

        @pl.when(owner > z)
        def _():
            up_copy(owner, h, at, wide).start()

        @pl.when(owner < z)
        def _():
            down_copy(owner, h, at, wide, z - 1).start()

    def reduce_both(k):
        each(0, 2, lambda at: [reduce(k, h, at, 1) for h in range(2)])
        each(2, 2 * groups, lambda at: reduce(k, None, at, 1))

    def at_end(k):
        owner = turn(z, k, planes)
        return (owner == 0) | (owner == planes - 1)

    def each(first, last, step):
        lax.fori_loop(first, last, lambda i, carry: (step(i), carry)[1], 0)

    with jax.named_scope("g00"):
        gather(0, 0)
    with jax.named_scope("qwait"):
        for sem in (load_sem, swap_recv):
            wait_for(qb.at[:tokens, : 2 * group_cols + key_cols], sem.at[0])
    with jax.named_scope("a0"):
        publish(0)
    with jax.named_scope("g01"):
        gather(0, 1)
    with jax.named_scope("qwait2"):
        for sem in (load_sem, swap_recv):
            wait_for(qb.at[:, group_cols:], sem.at[1])
    with jax.named_scope("a123"):
        each(1, groups, publish)
    later = [lambda i=i: gather(i // 2, i % 2) for i in range(2, 2 * planes)]

    def next_gather():
        if later:
            with jax.named_scope("gnext"):
                later.pop(0)()

    for g in range(groups):
        with jax.named_scope(f"pass{g}"):
            pass_on(g)
        if g == 0:
            with jax.named_scope("took00"):
                took(0, 0)
        with jax.named_scope(f"red0_{g}own"):
            reduce(0, None if g else 0, 2 * g, 1)
        if g == 0:
            next_gather()
        with jax.named_scope(f"arr{g}"):
            arrived(g)
        with jax.named_scope(f"red0_{g}other"):
            reduce(0, None if g else 0, 2 * g + 1, 1)
            if g == 0:
                with jax.named_scope("took01"):
                    took(0, 1)
                reduce(0, 1, 0, 1)
                reduce(0, 1, 1, 1)
        if g == 0:
            next_gather()
        if g < groups - 1:
            next_gather()

    def rest(k, between=None):
        def half_of(h):
            with jax.named_scope("took"):
                took(k, h)

            @pl.when(jnp.logical_not(at_end(k)))
            def _():
                with jax.named_scope("red"):
                    each(0, groups, lambda g: reduce(k, h, 2 * g, 2))

        half_of(0)
        if between is not None:
            between()
        half_of(1)

        @pl.when(at_end(k))
        def _():
            with jax.named_scope("redend"):
                reduce_both(k)

    rest(1, lambda: each(2 * planes - len(later), 2 * planes, lambda i: gather(i // 2, i % 2)))
    each(2, planes, rest)

    with jax.named_scope("t0"):
        for ref in (qb, gb, kb):
            wait_for(ref.at[:tokens], swap_send)
        wait_for(send.at[:, 1:], a2a_send)
        wait_for(vg.at[: (inner - 1) * length, : groups * HD], ag_send)
        wait_for(vg.at[:, : groups * HD], fwd_send)
    with jax.named_scope("t3"):
        wait_for(part.at[1:], rs_send)


def body(activations, queries, keys, out_grad, layout):
    members = lax.axis_size("dp")
    tokens, width = activations.shape
    inner = 1 << ((members.bit_length() - 1) // 2)
    planes = members // inner
    rows = layout.shape[0] // (members * SEQ)
    kv_width = keys.shape[1]
    groups = kv_width // SEQ // HD
    length = SEQ * tokens
    dma = pltpu.SemaphoreType.DMA
    operands = (activations, queries, keys, out_grad, layout)
    return pl.pallas_call(
        functools.partial(fused_kernel, planes=planes, inner=inner),
        out_shape=jax.ShapeDtypeStruct((rows, kv_width), jnp.float32),
        in_specs=[pl.BlockSpec(memory_space=pltpu.HBM)] * len(operands),
        out_specs=pl.BlockSpec(memory_space=pltpu.VMEM),
        scratch_shapes=[
            pltpu.VMEM((tokens, width), jnp.bfloat16),
            pltpu.VMEM((width, tokens), jnp.float32),
            pltpu.VMEM((rows // 2, tokens), jnp.float32),
            pltpu.SMEM(layout.shape, jnp.int32),
            pltpu.VMEM((length, queries.shape[1] // SEQ), jnp.bfloat16),
            pltpu.VMEM((length, kv_width // SEQ), jnp.bfloat16),
            pltpu.VMEM((length, queries.shape[1] // SEQ), jnp.bfloat16),
            pltpu.VMEM((planes, inner * SEQ, rows, tokens), jnp.bfloat16),
            pltpu.VMEM((planes, rows, inner * length), jnp.bfloat16),
            pltpu.VMEM((inner * length, kv_width), jnp.bfloat16),
            pltpu.VMEM((planes, rows, kv_width), jnp.bfloat16),
            pltpu.VMEM((planes, rows, kv_width), jnp.bfloat16),
            pltpu.VMEM((planes, rows, kv_width), jnp.bfloat16),
            pltpu.VMEM((rows, SEQ * HD), jnp.float32),
            dma((4,)),
            dma(()),
            dma((2,)),
            dma(()),
            dma((2,)),
            dma(()),
            dma((planes, 2)),
            dma(()),
            dma((groups,)),
            dma(()),
            dma((groups,)),
            dma(()),
            dma((planes - 1, 2, groups)),
            dma((2, 2 * groups + 2)),
        ],
        compiler_params=pltpu.CompilerParams(
            collective_id=0, has_side_effects=True, vmem_limit_bytes=32 * 2**20
        ),
    )(*(pltpu.with_memory_space_constraint(x, pltpu.HBM) for x in operands))


def solution(mesh):
    whole = ("dp", "seq")
    return jax.shard_map(
        body,
        mesh=mesh,
        in_specs=(P(whole, None),) * 4 + (P(),),
        out_specs=P(whole, None),
        check_vma=False,
    )
```

```python
import functools
import math

import jax
import jax.numpy as jnp
from jax import lax
from jax.experimental import pallas as pl
from jax.experimental.pallas import tpu as pltpu
from jax.sharding import PartitionSpec as P

H = 64
KVH = 8
HD = 128
SEQ = 2
MESH = pl.DeviceIdType.MESH


def relative(place, step, bits):
    total = 0
    for b in range(bits):
        total = total + (place // (1 << b) + step // (1 << b)) % 2 * (1 << b)
    return total


def fused_kernel(
    act_hbm, q_hbm, k_hbm, grad_hbm, layout_hbm, out_ref,
    act, flipped, picked, lay, qb, kb, gb, send, held, vg, line_in, part, acc,
    act_sem, lay_sem, load_sem, swap_send, swap_recv, a2a_send, a2a_recv, ag_send, ag_recv,
    fwd_send, fwd_recv, rs_send, line_sem, *, group_masks, line_masks,
):
    tokens, width = act_hbm.shape
    rows = out_ref.shape[0]
    bits = len(group_masks) + len(line_masks)
    inner, sets = 1 << len(group_masks), 1 << len(line_masks)
    me, core = lax.axis_index("dp"), lax.axis_index("seq")
    other = 1 - core
    heads_cols, key_cols = q_hbm.shape[1] // SEQ, k_hbm.shape[1] // SEQ
    length = SEQ * tokens
    per_group = H // KVH
    groups = key_cols // HD
    half = rows // 2
    group_cols = per_group * HD
    stretch = width // 4

    moves = [mask * (1 - me // mask % 2 * 2) for mask in group_masks]

    def member(step):
        return me + sum(step // (1 << i) % 2 * move for i, move in enumerate(moves))

    def across(place, step):
        for i, mask in enumerate(line_masks):
            if step >> i & 1:
                for b in range(bits):
                    if mask >> b & 1:
                        place = place + (1 << b) * (1 - place // (1 << b) % 2 * 2)
        return place

    here_at = sum(me // mask % 2 * (1 << i) for i, mask in enumerate(group_masks))
    place = here_at * SEQ + core

    cuts = ((k_hbm, kb, key_cols, 0, key_cols),) + tuple(
        (source, target, heads_cols, first, last - first)
        for first, last in ((0, group_cols), (group_cols, heads_cols))
        for source, target in ((q_hbm, qb), (grad_hbm, gb))
    )

    early_cuts = 3

    def cut(i, of_core):
        source, target, cols, first, count = cuts[i]
        return (
            source.at[:, pl.ds(pl.multiple_of(of_core * cols + first, 128), count)],
            target.at[pl.ds(pl.multiple_of(core * tokens, 128), tokens), pl.ds(first, count)],
        )

    flips = [
        pltpu.make_async_copy(
            act_hbm.at[:, pl.ds(i * stretch, stretch)],
            act.at[:, pl.ds(i * stretch, stretch)],
            act_sem.at[i],
        )
        for i in range(width // stretch)
    ]
    lay_load = pltpu.make_async_copy(layout_hbm, lay, lay_sem)
    loads = [pltpu.make_async_copy(*cut(i, core), load_sem.at[int(i >= early_cuts)]) for i in range(len(cuts))]
    for load in [*flips, lay_load]:
        load.start()

    barrier = pltpu.get_barrier_semaphore()
    peers = [(member(j // SEQ), (core + j) % SEQ) for j in range(1, inner * SEQ)]
    peers += [(across(me, 1 << i), core) for i in range(len(line_masks))]
    for to in peers:
        pl.semaphore_signal(barrier, inc=1, device_id=to, device_id_type=MESH)

    swaps = []
    for i in range(len(cuts)):
        source, target = cut(i, other)
        swaps.append(
            pltpu.make_async_remote_copy(
                src_ref=source, dst_ref=target, send_sem=swap_send, recv_sem=swap_recv.at[int(i >= early_cuts)],
                device_id=(me, other), device_id_type=MESH,
            )
        )
    step = 2048

    def flip(i, carry):
        at = pl.multiple_of(i * step, step)
        flipped[pl.ds(at, step), :] = act[:, pl.ds(at, step)].T.astype(jnp.float32)
        return carry

    for i, load in enumerate(flips):
        with jax.named_scope("act_wait"):
            load.wait()
        if i == 0:
            for other_load in loads:
                other_load.start()
        with jax.named_scope("flip"):
            lax.fori_loop(i * stretch // step, (i + 1) * stretch // step, flip, 0)
        if i == 1:
            with jax.named_scope("barrier"):
                pl.semaphore_wait(barrier, len(peers))
            for swap in swaps:
                swap.start()
    lay_load.wait()

    def wait_for(like, sem):
        pltpu.make_async_remote_copy(
            src_ref=like, dst_ref=like, send_sem=sem, recv_sem=sem,
            device_id=(me, other), device_id_type=MESH,
        ).wait_recv()

    def pick(first_row):
        def some(i, carry):
            first = pl.multiple_of(i * 32, 32)
            for r in range(32):
                row = lay[first_row + first + r]
                picked[pl.ds(first + r, 1), :] = flipped[pl.ds(row, 1), :]
            return carry

        lax.fori_loop(0, half // 32, some, 0)

    def held_piece(s, h):
        return held.at[
            s,
            pl.ds(pl.multiple_of(h * half, 16), half),
            pl.ds(pl.multiple_of(place * tokens, 128), tokens),
        ]

    def block(s, h, j):
        return pltpu.make_async_remote_copy(
            src_ref=send.at[s, j, pl.ds(pl.multiple_of(h * half, 16), half)],
            dst_ref=held_piece(s, h),
            send_sem=a2a_send,
            recv_sem=a2a_recv.at[s, h],
            device_id=(member(j // SEQ), (core + j) % SEQ),
            device_id_type=MESH,
        )

    def gather(s, h, start=True):
        def first_row(j):
            owner = across(member(j // SEQ), s)
            return (owner * SEQ + (core + j) % SEQ) * rows + h * half

        def to(i, carry):
            j = inner * SEQ - i
            pick(first_row(j))
            send[s, j, pl.ds(pl.multiple_of(h * half, 16), half)] = picked[...].astype(jnp.bfloat16)
            if start:
                block(s, h, j).start()
            return carry

        lax.fori_loop(1, inner * SEQ, to, 0)
        pick(first_row(0))
        held_piece(s, h)[...] = picked[...].astype(jnp.bfloat16)

    def release(s, h):
        lax.fori_loop(1, inner * SEQ, lambda i, carry: (block(s, h, inner * SEQ - i).start(), carry)[1], 0)

    def took(s, h):
        wait_for(send.at[0, 1:, :half], a2a_recv.at[s, h])

    scale = math.log2(math.e) / float(HD) ** 0.5
    key_at = lax.broadcasted_iota(jnp.int32, (tokens, 2 * tokens), 0)
    query_at = lax.broadcasted_iota(jnp.int32, (tokens, 2 * tokens), 1) % tokens
    allowed = key_at <= query_at

    def weights_of(scores):
        powers = jnp.exp2((scores - jnp.max(scores, axis=0, keepdims=True)) * scale)
        return (powers * (1.0 / jnp.sum(powers, axis=0, keepdims=True))).astype(jnp.bfloat16)

    def stacked(ref, row, col):
        return jnp.concatenate(
            [
                ref[row : row + tokens, pl.ds(pl.multiple_of(col, 128), HD)],
                ref[row : row + tokens, pl.ds(pl.multiple_of(col + HD, 128), HD)],
            ],
            axis=0,
        )

    def attend(g):
        keys = kb[:, pl.ds(pl.multiple_of(g * HD, 128), HD)]
        early = jnp.zeros((tokens, HD), jnp.float32)
        both = jnp.zeros((length, HD), jnp.float32)
        for pair in range(per_group // 2):
            col = (g * per_group + 2 * pair) * HD
            against = (((1,), (1,)), ((), ()))
            first = lax.dot_general(
                keys[:tokens], stacked(qb, 0, col), against, preferred_element_type=jnp.float32
            )
            second = lax.dot_general(
                keys, stacked(qb, tokens, col), against, preferred_element_type=jnp.float32
            )
            first = jnp.where(allowed, first, -jnp.inf)
            second = jnp.concatenate(
                [second[:tokens], jnp.where(allowed, second[tokens:], -jnp.inf)], axis=0
            )
            early += jnp.dot(
                weights_of(first), stacked(gb, 0, col), preferred_element_type=jnp.float32
            )
            both += jnp.dot(
                weights_of(second), stacked(gb, tokens, col), preferred_element_type=jnp.float32
            )
        done = jnp.concatenate([both[:tokens] + early, both[tokens:]], axis=0)
        grads(0, 2 * g)[...] = done.astype(jnp.bfloat16)

    def grads(step, at):
        from_at = relative(here_at, step, len(group_masks))
        return vg.at[
            pl.ds(pl.multiple_of(from_at * length, 128), length),
            pl.ds(pl.multiple_of(at * HD, 128), HD),
        ]

    def gather_copy(g, step, i):
        return pltpu.make_async_remote_copy(
            src_ref=grads(step, 2 * g), dst_ref=grads(step, 2 * g),
            send_sem=ag_send, recv_sem=ag_recv.at[g, step + (1 << i)],
            device_id=(member(1 << i), core), device_id_type=MESH,
        )

    def forward_copy(g, step):
        return pltpu.make_async_remote_copy(
            src_ref=grads(step, 2 * g), dst_ref=grads(step, 2 * g + 1),
            send_sem=fwd_send, recv_sem=fwd_recv.at[g],
            device_id=(me, other), device_id_type=MESH,
        )

    def direct_copy(g, step):
        return pltpu.make_async_remote_copy(
            src_ref=grads(0, 2 * g), dst_ref=grads(0, 2 * g),
            send_sem=ag_send, recv_sem=ag_recv.at[g, step],
            device_id=(member(step), core), device_id_type=MESH,
        )

    def publish(g, direct=False):
        attend(g)
        if direct:
            for step in reversed(range(1, inner)):
                direct_copy(g, step).start()
        else:
            for i in reversed(range(len(group_masks))):
                gather_copy(g, 0, i).start()
        forward_copy(g, 0).start()

    def pass_on(g, step, relay=True):
        wait_for(vg.at[:length, :HD], ag_recv.at[g, step])
        lowest = (step & -step).bit_length() - 1
        if relay:
            for i in reversed(range(lowest)):
                gather_copy(g, step, i).start()
        forward_copy(g, step).start()

    near_steps = [1 << i for i in reversed(range(len(group_masks)))]
    far_steps = sorted(
        (step for step in range(1, inner) if step not in near_steps), key=lambda step: (bin(step).count("1"), -step)
    )

    def arrived(g):
        wait_for(vg.at[:, :HD], fwd_recv.at[g])

    def slot(ref, s, h, g):
        return ref.at[
            s,
            pl.ds(pl.multiple_of(h * half, 16), half),
            pl.ds(pl.multiple_of(g * SEQ * HD, 128), SEQ * HD),
        ]

    def line_copy(s, h, g):
        lowest = (s & -s).bit_length() - 1
        return pltpu.make_async_remote_copy(
            src_ref=slot(part, s - 1, h, g), dst_ref=slot(line_in, s - 1, h, g),
            send_sem=rs_send, recv_sem=line_sem.at[s - 1, h, g],
            device_id=(across(me, 1 << lowest), core), device_id_type=MESH,
        )

    def reduce(s, h, g):
        at_rows = pl.ds(pl.multiple_of(h * half, 16), half)
        cols = pl.ds(pl.multiple_of(g * SEQ * HD, 128), SEQ * HD)
        acc[...] = jnp.dot(held[s, at_rows, :], vg[:, cols], preferred_element_type=jnp.float32)
        lowest = (s & -s).bit_length() - 1 if s else len(line_masks)
        for i in range(lowest):
            line_copy(s + (1 << i), h, g).wait_recv()
            acc[...] += slot(line_in, s + (1 << i) - 1, h, g)[...].astype(jnp.float32)
        if s:
            slot(part, s - 1, h, g)[...] = acc[...].astype(jnp.bfloat16)
            line_copy(s, h, g).start()
        else:
            for c in range(SEQ):
                of_core = (core + c) % SEQ
                out_ref[at_rows, pl.ds(pl.multiple_of((of_core * groups + g) * HD, 128), HD)] = acc[
                    :, c * HD : (c + 1) * HD
                ]

    def each(first, last, step):
        lax.fori_loop(first, last, lambda i, carry: (step(i), carry)[1], 0)

    order = [(sets - 1, 0), (sets - 2, 0), (sets - 1, 1), (sets - 2, 1)]
    order += [(s, h) for s in reversed(range(sets - 2)) for h in range(2)]
    later = order[3:]

    def next_gather():
        if later:
            with jax.named_scope("gnext"):
                gather(*later.pop(0))

    def pass_near(g):
        with jax.named_scope(f"pass{g}"):
            for step in near_steps:
                pass_on(g, step)

    def pass_far(g):
        with jax.named_scope(f"far{g}"):
            for step in far_steps:
                pass_on(g, step)

    def first(g):
        with jax.named_scope(f"arr{g}"):
            arrived(g)
        with jax.named_scope(f"redfirst{g}"):
            reduce(sets - 1, 0, g)

    def second(g):
        with jax.named_scope(f"redsecond{g}"):
            reduce(sets - 2, 0, g)

    with jax.named_scope("g00"):
        gather(*order[0])
    with jax.named_scope("qwait"):
        for sem in (load_sem, swap_recv):
            wait_for(qb.at[:tokens, : 2 * group_cols + key_cols], sem.at[0])
    with jax.named_scope("a0"):
        publish(0, True)
    with jax.named_scope("g01"):
        gather(*order[1])
    for sem in (load_sem, swap_recv):
        wait_for(qb.at[:, group_cols:], sem.at[1])
    with jax.named_scope("a123"):
        each(1, groups, publish)
    with jax.named_scope("pass0"):
        for step in range(1, inner):
            pass_on(0, step, False)
    with jax.named_scope("held"):
        gather(*order[2], False)
    took(*order[0])
    first(0)
    for g in range(1, groups):
        pass_near(g)
        if g == 2:
            took(*order[1])
            second(0)
    release(*order[2])
    next_gather()
    pass_far(1)
    first(1)
    for g in range(2, groups):
        pass_far(g)
        next_gather()
        first(g)
        second(g - 1)

    def rest(s, h):
        with jax.named_scope("took"):
            took(s, h)
        with jax.named_scope(f"red{s}{h}"):
            each(0, groups, lambda g: reduce(s, h, g))

    rest(*order[2])
    second(groups - 1)
    while later:
        next_gather()
    rest(*order[3])
    for s, h in order[4:]:
        rest(s, h)

    with jax.named_scope("t0"):
        for ref in (qb, gb, kb):
            wait_for(ref.at[:tokens], swap_send)
        wait_for(send.at[:, 1:], a2a_send)
        wait_for(vg.at[: (inner - 1) * length, : groups * HD], ag_send)
        wait_for(vg.at[:, : groups * HD], fwd_send)
    with jax.named_scope("t3"):
        wait_for(part, rs_send)


def body(activations, queries, keys, out_grad, layout):
    members = lax.axis_size("dp")
    tokens, width = activations.shape
    bits = members.bit_length() - 1
    group_masks = [1 << b for b in range(0, bits, 2)]
    line_masks = [1 << b for b in range(1, bits, 2)]
    line_masks[-1] += line_masks[-1] // 2
    inner, sets = 1 << len(group_masks), 1 << len(line_masks)
    rows = layout.shape[0] // (members * SEQ)
    kv_width = keys.shape[1]
    groups = kv_width // SEQ // HD
    length = SEQ * tokens
    dma = pltpu.SemaphoreType.DMA
    operands = (activations, queries, keys, out_grad, layout)
    return pl.pallas_call(
        functools.partial(fused_kernel, group_masks=group_masks, line_masks=line_masks),
        out_shape=jax.ShapeDtypeStruct((rows, kv_width), jnp.float32),
        in_specs=[pl.BlockSpec(memory_space=pltpu.HBM)] * len(operands),
        out_specs=pl.BlockSpec(memory_space=pltpu.VMEM),
        scratch_shapes=[
            pltpu.VMEM((tokens, width), jnp.bfloat16),
            pltpu.VMEM((width, tokens), jnp.float32),
            pltpu.VMEM((rows // 2, tokens), jnp.float32),
            pltpu.SMEM(layout.shape, jnp.int32),
            pltpu.VMEM((length, queries.shape[1] // SEQ), jnp.bfloat16),
            pltpu.VMEM((length, kv_width // SEQ), jnp.bfloat16),
            pltpu.VMEM((length, queries.shape[1] // SEQ), jnp.bfloat16),
            pltpu.VMEM((sets, inner * SEQ, rows, tokens), jnp.bfloat16),
            pltpu.VMEM((sets, rows, inner * length), jnp.bfloat16),
            pltpu.VMEM((inner * length, kv_width), jnp.bfloat16),
            pltpu.VMEM((sets - 1, rows, kv_width), jnp.bfloat16),
            pltpu.VMEM((sets - 1, rows, kv_width), jnp.bfloat16),
            pltpu.VMEM((rows // 2, SEQ * HD), jnp.float32),
            dma((4,)),
            dma(()),
            dma((2,)),
            dma(()),
            dma((2,)),
            dma(()),
            dma((sets, 2)),
            dma(()),
            dma((groups, inner)),
            dma(()),
            dma((groups,)),
            dma(()),
            dma((sets - 1, 2, groups)),
        ],
        compiler_params=pltpu.CompilerParams(
            collective_id=0, has_side_effects=True, vmem_limit_bytes=32 * 2**20
        ),
    )(*(pltpu.with_memory_space_constraint(x, pltpu.HBM) for x in operands))


def solution(mesh):
    whole = ("dp", "seq")
    return jax.shard_map(
        body,
        mesh=mesh,
        in_specs=(P(whole, None),) * 4 + (P(),),
        out_specs=P(whole, None),
        check_vma=False,
    )
```

```python
import functools
import math

import jax
import jax.numpy as jnp
from jax import lax
from jax.experimental import pallas as pl
from jax.experimental.pallas import tpu as pltpu
from jax.sharding import PartitionSpec as P

H = 64
KVH = 8
HD = 128
SEQ = 2
MESH = pl.DeviceIdType.MESH


def relative(place, step, bits):
    total = 0
    for b in range(bits):
        total = total + (place // (1 << b) + step // (1 << b)) % 2 * (1 << b)
    return total


def turn(z, k, count):
    above = count - 1 - z
    sign = jnp.where(above >= z, 1, -1)
    big, small = jnp.maximum(above, z), jnp.minimum(above, z)
    later = k - (big - small)
    lone = later < 0
    distance = jnp.where(lone, big - k, small - later // 2)
    side = jnp.where(lone | (later % 2 == 1), sign, -sign)
    return z + side * distance


def fused_kernel(
    act_hbm, q_hbm, k_hbm, grad_hbm, layout_hbm, out_ref,
    act, flipped, picked, lay, qb, kb, gb, send, held, vg, down_in, up_in, part, acc,
    act_sem, lay_sem, load_sem, swap_send, swap_recv, a2a_send, a2a_recv, ag_send, ag_recv,
    fwd_send, fwd_recv, rs_send, line_sem, end_sem, *, planes, inner,
):
    tokens, width = act_hbm.shape
    rows = out_ref.shape[0]
    bits = inner.bit_length() - 1
    me, core = lax.axis_index("dp"), lax.axis_index("seq")
    z, p = me // inner, me % inner
    other = 1 - core
    heads_cols, key_cols = q_hbm.shape[1] // SEQ, k_hbm.shape[1] // SEQ
    length = SEQ * tokens
    per_group = H // KVH
    groups = key_cols // HD
    half = rows // 2
    place = p * SEQ + core
    group_cols = per_group * HD
    stretch = width // 4

    cuts = ((k_hbm, kb, key_cols, 0, key_cols),) + tuple(
        (source, target, heads_cols, first, last - first)
        for first, last in ((0, group_cols), (group_cols, heads_cols))
        for source, target in ((q_hbm, qb), (grad_hbm, gb))
    )

    early_cuts = 3

    def cut(i, of_core):
        source, target, cols, first, count = cuts[i]
        return (
            source.at[:, pl.ds(pl.multiple_of(of_core * cols + first, 128), count)],
            target.at[pl.ds(pl.multiple_of(core * tokens, 128), tokens), pl.ds(first, count)],
        )

    flips = [
        pltpu.make_async_copy(
            act_hbm.at[:, pl.ds(i * stretch, stretch)],
            act.at[:, pl.ds(i * stretch, stretch)],
            act_sem.at[i],
        )
        for i in range(width // stretch)
    ]
    lay_load = pltpu.make_async_copy(layout_hbm, lay, lay_sem)
    loads = [pltpu.make_async_copy(*cut(i, core), load_sem.at[int(i >= early_cuts)]) for i in range(len(cuts))]
    for load in [*flips, lay_load]:
        load.start()

    barrier = pltpu.get_barrier_semaphore()
    for j in range(1, inner * SEQ):
        to = (z * inner + relative(p, j // SEQ, bits), (core + j) % SEQ)
        pl.semaphore_signal(barrier, inc=1, device_id=to, device_id_type=MESH)

    @pl.when(z > 0)
    def _():
        pl.semaphore_signal(barrier, inc=1, device_id=(me - inner, core), device_id_type=MESH)

    @pl.when(z < planes - 1)
    def _():
        pl.semaphore_signal(barrier, inc=1, device_id=(me + inner, core), device_id_type=MESH)

    near = inner * SEQ - 1 + jnp.where(z > 0, 1, 0) + jnp.where(z < planes - 1, 1, 0)

    swaps = []
    for i in range(len(cuts)):
        source, target = cut(i, other)
        swaps.append(
            pltpu.make_async_remote_copy(
                src_ref=source, dst_ref=target, send_sem=swap_send, recv_sem=swap_recv.at[int(i >= early_cuts)],
                device_id=(me, other), device_id_type=MESH,
            )
        )
    step = 2048

    def flip(i, carry):
        at = pl.multiple_of(i * step, step)
        flipped[pl.ds(at, step), :] = act[:, pl.ds(at, step)].T.astype(jnp.float32)
        return carry

    for i, load in enumerate(flips):
        with jax.named_scope("act_wait"):
            load.wait()
        if i == 0:
            for other_load in loads:
                other_load.start()
        with jax.named_scope("flip"):
            lax.fori_loop(i * stretch // step, (i + 1) * stretch // step, flip, 0)
        if i == 1:
            with jax.named_scope("barrier"):
                pl.semaphore_wait(barrier, near)
            for swap in swaps:
                swap.start()
    lay_load.wait()

    def wait_for(like, sem):
        pltpu.make_async_remote_copy(
            src_ref=like, dst_ref=like, send_sem=sem, recv_sem=sem,
            device_id=(me, other), device_id_type=MESH,
        ).wait_recv()

    def pick(first_row):
        def some(i, carry):
            first = pl.multiple_of(i * 32, 32)
            for r in range(32):
                row = lay[first_row + first + r]
                picked[pl.ds(first + r, 1), :] = flipped[pl.ds(row, 1), :]
            return carry

        lax.fori_loop(0, half // 32, some, 0)

    def held_piece(owner, h):
        return held.at[
            owner,
            pl.ds(pl.multiple_of(h * half, 16), half),
            pl.ds(pl.multiple_of(place * tokens, 128), tokens),
        ]

    def block(k, h, j):
        to_p, to_core = relative(p, j // SEQ, bits), (core + j) % SEQ
        return pltpu.make_async_remote_copy(
            src_ref=send.at[k, j, pl.ds(pl.multiple_of(h * half, 16), half)],
            dst_ref=held_piece(turn(z, k, planes), h),
            send_sem=a2a_send,
            recv_sem=a2a_recv.at[k, h],
            device_id=(z * inner + to_p, to_core),
            device_id_type=MESH,
        )

    def gather(k, h):
        owner = turn(z, k, planes)

        def first_row(to_p, to_core):
            return ((owner * inner + to_p) * SEQ + to_core) * rows + h * half

        def to(i, carry):
            j = jnp.where(i <= 4, inner * SEQ - 1 - (i - 1) % 2 * 2 - (i - 1) // 2, inner * SEQ - i)
            pick(first_row(relative(p, j // SEQ, bits), (core + j) % SEQ))
            send[k, j, pl.ds(pl.multiple_of(h * half, 16), half)] = picked[...].astype(jnp.bfloat16)
            block(k, h, j).start()
            return carry

        lax.fori_loop(1, inner * SEQ, to, 0)
        pick(first_row(p, core))
        held_piece(owner, h)[...] = picked[...].astype(jnp.bfloat16)

    def took(k, h):
        wait_for(send.at[0, 1:, :half], a2a_recv.at[k, h])

    scale = math.log2(math.e) / float(HD) ** 0.5
    key_at = lax.broadcasted_iota(jnp.int32, (tokens, 2 * tokens), 0)
    query_at = lax.broadcasted_iota(jnp.int32, (tokens, 2 * tokens), 1) % tokens
    allowed = key_at <= query_at

    def weights_of(scores):
        powers = jnp.exp2((scores - jnp.max(scores, axis=0, keepdims=True)) * scale)
        return (powers * (1.0 / jnp.sum(powers, axis=0, keepdims=True))).astype(jnp.bfloat16)

    def stacked(ref, row, col):
        return jnp.concatenate(
            [
                ref[row : row + tokens, pl.ds(pl.multiple_of(col, 128), HD)],
                ref[row : row + tokens, pl.ds(pl.multiple_of(col + HD, 128), HD)],
            ],
            axis=0,
        )

    def grads(from_p, at):
        return vg.at[
            pl.ds(pl.multiple_of(from_p * length, 128), length),
            pl.ds(pl.multiple_of(at * HD, 128), HD),
        ]

    def attend(g):
        keys = kb[:, pl.ds(pl.multiple_of(g * HD, 128), HD)]
        early = jnp.zeros((tokens, HD), jnp.float32)
        both = jnp.zeros((length, HD), jnp.float32)
        for pair in range(per_group // 2):
            col = (g * per_group + 2 * pair) * HD
            against = (((1,), (1,)), ((), ()))
            first = lax.dot_general(
                keys[:tokens], stacked(qb, 0, col), against, preferred_element_type=jnp.float32
            )
            second = lax.dot_general(
                keys, stacked(qb, tokens, col), against, preferred_element_type=jnp.float32
            )
            first = jnp.where(allowed, first, -jnp.inf)
            second = jnp.concatenate(
                [second[:tokens], jnp.where(allowed, second[tokens:], -jnp.inf)], axis=0
            )
            early += jnp.dot(
                weights_of(first), stacked(gb, 0, col), preferred_element_type=jnp.float32
            )
            both += jnp.dot(
                weights_of(second), stacked(gb, tokens, col), preferred_element_type=jnp.float32
            )
        done = jnp.concatenate([both[:tokens] + early, both[tokens:]], axis=0)
        grads(p, 2 * g)[...] = done.astype(jnp.bfloat16)

    def gather_copy(g, jp):
        return pltpu.make_async_remote_copy(
            src_ref=grads(p, 2 * g), dst_ref=grads(p, 2 * g),
            send_sem=ag_send, recv_sem=ag_recv.at[g],
            device_id=(z * inner + relative(p, jp, bits), core), device_id_type=MESH,
        )

    def forward_copy(g, jp):
        from_p = relative(p, jp, bits)
        return pltpu.make_async_remote_copy(
            src_ref=grads(from_p, 2 * g), dst_ref=grads(from_p, 2 * g + 1),
            send_sem=fwd_send, recv_sem=fwd_recv.at[g],
            device_id=(me, other), device_id_type=MESH,
        )

    def publish(g):
        attend(g)
        for jp in reversed(range(1, inner)):
            gather_copy(g, jp).start()
        forward_copy(g, 0).start()

    def pass_on(g):
        wait_for(vg.at[: (inner - 1) * length, :HD], ag_recv.at[g])
        for jp in range(1, inner):
            forward_copy(g, jp).start()

    def arrived(g):
        wait_for(vg.at[:, :HD], fwd_recv.at[g])

    def slot(ref, owner, h, at, wide):
        count = rows if h is None else half
        first = 0 if h is None else pl.multiple_of(h * half, 16)
        return ref.at[owner, pl.ds(first, count), pl.ds(pl.multiple_of(at * HD, 128), wide * HD)]

    def end_sem_of(end, h, at):
        return end_sem.at[end, at if h is None or h == 0 else 2 * groups + at]

    def up_copy(owner, h, at, wide):
        sem = end_sem_of(1, h, at) if wide == 1 else line_sem.at[owner - 1, h, at // 2]
        return pltpu.make_async_remote_copy(
            src_ref=slot(part, owner, h, at, wide), dst_ref=slot(up_in, owner, h, at, wide),
            send_sem=rs_send, recv_sem=sem,
            device_id=(me + inner, core), device_id_type=MESH,
        )

    def down_copy(owner, h, at, wide, to):
        if wide == 1:
            sem = end_sem_of(0, h, at)
        else:
            sem = line_sem.at[jnp.where(owner == to, planes, owner) - 1 - jnp.where(owner == to, 1, 0), h, at // 2]
        return pltpu.make_async_remote_copy(
            src_ref=slot(part, owner, h, at, wide), dst_ref=slot(down_in, owner, h, at, wide),
            send_sem=rs_send, recv_sem=sem,
            device_id=(me - inner, core), device_id_type=MESH,
        )

    def reduce(k, h, at, wide):
        owner = turn(z, k, planes)
        count = rows if h is None else half
        at_rows = pl.ds(0 if h is None else pl.multiple_of(h * half, 16), count)
        cols = pl.ds(pl.multiple_of(at * HD, 128), wide * HD)
        here = acc.at[:count, : wide * HD]
        here[...] = jnp.dot(held[owner, at_rows, :], vg[:, cols], preferred_element_type=jnp.float32)

        @pl.when((owner >= z) & (z > 0))
        def _():
            up_copy(owner, h, at, wide).wait_recv()
            here[...] += slot(up_in, owner, h, at, wide)[...].astype(jnp.float32)

        @pl.when((owner <= z) & (z < planes - 1))
        def _():
            down_copy(owner, h, at, wide, z).wait_recv()
            here[...] += slot(down_in, owner, h, at, wide)[...].astype(jnp.float32)

        @pl.when(owner == z)
        def _():
            for c in range(wide):
                of_core = (core + at + c) % SEQ
                out_ref[at_rows, pl.ds(pl.multiple_of((of_core * groups + (at + c) // 2) * HD, 128), HD)] = acc[
                    :count, c * HD : (c + 1) * HD
                ]

        @pl.when(owner != z)
        def _():
            slot(part, owner, h, at, wide)[...] = here[...].astype(jnp.bfloat16)

        @pl.when(owner > z)
        def _():
            up_copy(owner, h, at, wide).start()

        @pl.when(owner < z)
        def _():
            down_copy(owner, h, at, wide, z - 1).start()

    def reduce_both(k):
        each(0, 2, lambda at: [reduce(k, h, at, 1) for h in range(2)])
        each(2, 2 * groups, lambda at: reduce(k, None, at, 1))

    def at_end(k):
        owner = turn(z, k, planes)
        return (owner == 0) | (owner == planes - 1)

    def each(first, last, step):
        lax.fori_loop(first, last, lambda i, carry: (step(i), carry)[1], 0)

    with jax.named_scope("g00"):
        gather(0, 0)
    with jax.named_scope("qwait"):
        for sem in (load_sem, swap_recv):
            wait_for(qb.at[:tokens, : 2 * group_cols + key_cols], sem.at[0])
    with jax.named_scope("a0"):
        publish(0)
    with jax.named_scope("g01"):
        gather(0, 1)
    with jax.named_scope("qwait2"):
        for sem in (load_sem, swap_recv):
            wait_for(qb.at[:, group_cols:], sem.at[1])
    with jax.named_scope("a123"):
        each(1, groups, publish)
    later = [lambda i=i: gather(i // 2, i % 2) for i in range(2, 2 * planes)]

    def next_gather():
        if later:
            with jax.named_scope("gnext"):
                later.pop(0)()

    for g in range(groups):
        with jax.named_scope(f"pass{g}"):
            pass_on(g)
        if g == 0:
            with jax.named_scope("took00"):
                took(0, 0)
        with jax.named_scope(f"red0_{g}own"):
            reduce(0, None if g else 0, 2 * g, 1)
        if g == 0:
            next_gather()
        with jax.named_scope(f"arr{g}"):
            arrived(g)
        with jax.named_scope(f"red0_{g}other"):
            reduce(0, None if g else 0, 2 * g + 1, 1)
            if g == 0:
                with jax.named_scope("took01"):
                    took(0, 1)
                reduce(0, 1, 0, 1)
                reduce(0, 1, 1, 1)
        if g == 0:
            next_gather()
        if g < groups - 1:
            next_gather()

    def rest(k, between=None):
        def half_of(h):
            with jax.named_scope("took"):
                took(k, h)

            @pl.when(jnp.logical_not(at_end(k)))
            def _():
                with jax.named_scope("red"):
                    each(0, groups, lambda g: reduce(k, h, 2 * g, 2))

        half_of(0)
        if between is not None:
            between()
        half_of(1)

        @pl.when(at_end(k))
        def _():
            with jax.named_scope("redend"):
                reduce_both(k)

    rest(1, lambda: each(2 * planes - len(later), 2 * planes, lambda i: gather(i // 2, i % 2)))
    each(2, planes, rest)

    with jax.named_scope("t0"):
        for ref in (qb, gb, kb):
            wait_for(ref.at[:tokens], swap_send)
        wait_for(send.at[:, 1:], a2a_send)
        wait_for(vg.at[: (inner - 1) * length, : groups * HD], ag_send)
        wait_for(vg.at[:, : groups * HD], fwd_send)
    with jax.named_scope("t3"):
        wait_for(part.at[1:], rs_send)


def body(activations, queries, keys, out_grad, layout):
    members = lax.axis_size("dp")
    tokens, width = activations.shape
    inner = 1 << ((members.bit_length() - 1) // 2)
    planes = members // inner
    rows = layout.shape[0] // (members * SEQ)
    kv_width = keys.shape[1]
    groups = kv_width // SEQ // HD
    length = SEQ * tokens
    dma = pltpu.SemaphoreType.DMA
    operands = (activations, queries, keys, out_grad, layout)
    return pl.pallas_call(
        functools.partial(fused_kernel, planes=planes, inner=inner),
        out_shape=jax.ShapeDtypeStruct((rows, kv_width), jnp.float32),
        in_specs=[pl.BlockSpec(memory_space=pltpu.HBM)] * len(operands),
        out_specs=pl.BlockSpec(memory_space=pltpu.VMEM),
        scratch_shapes=[
            pltpu.VMEM((tokens, width), jnp.bfloat16),
            pltpu.VMEM((width, tokens), jnp.float32),
            pltpu.VMEM((rows // 2, tokens), jnp.float32),
            pltpu.SMEM(layout.shape, jnp.int32),
            pltpu.VMEM((length, queries.shape[1] // SEQ), jnp.bfloat16),
            pltpu.VMEM((length, kv_width // SEQ), jnp.bfloat16),
            pltpu.VMEM((length, queries.shape[1] // SEQ), jnp.bfloat16),
            pltpu.VMEM((planes, inner * SEQ, rows, tokens), jnp.bfloat16),
            pltpu.VMEM((planes, rows, inner * length), jnp.bfloat16),
            pltpu.VMEM((inner * length, kv_width), jnp.bfloat16),
            pltpu.VMEM((planes, rows, kv_width), jnp.bfloat16),
            pltpu.VMEM((planes, rows, kv_width), jnp.bfloat16),
            pltpu.VMEM((planes, rows, kv_width), jnp.bfloat16),
            pltpu.VMEM((rows, SEQ * HD), jnp.float32),
            dma((4,)),
            dma(()),
            dma((2,)),
            dma(()),
            dma((2,)),
            dma(()),
            dma((planes, 2)),
            dma(()),
            dma((groups,)),
            dma(()),
            dma((groups,)),
            dma(()),
            dma((planes - 1, 2, groups)),
            dma((2, 2 * groups + 2)),
        ],
        compiler_params=pltpu.CompilerParams(
            collective_id=0, has_side_effects=True, vmem_limit_bytes=32 * 2**20
        ),
    )(*(pltpu.with_memory_space_constraint(x, pltpu.HBM) for x in operands))


def solution(mesh):
    whole = ("dp", "seq")
    return jax.shard_map(
        body,
        mesh=mesh,
        in_specs=(P(whole, None),) * 4 + (P(),),
        out_specs=P(whole, None),
        check_vma=False,
    )
```

```python
import functools
import math

import jax
import jax.numpy as jnp
from jax import lax
from jax.experimental import pallas as pl
from jax.experimental.pallas import tpu as pltpu
from jax.sharding import PartitionSpec as P

H = 64
KVH = 8
HD = 128
SEQ = 2
MESH = pl.DeviceIdType.MESH


def relative(place, step, bits):
    total = 0
    for b in range(bits):
        total = total + (place // (1 << b) + step // (1 << b)) % 2 * (1 << b)
    return total


def turn(z, k, count):
    above = count - 1 - z
    sign = jnp.where(above >= z, 1, -1)
    big, small = jnp.maximum(above, z), jnp.minimum(above, z)
    later = k - (big - small)
    lone = later < 0
    distance = jnp.where(lone, big - k, small - later // 2)
    side = jnp.where(lone | (later % 2 == 1), sign, -sign)
    return z + side * distance


def fused_kernel(
    act_hbm, q_hbm, k_hbm, grad_hbm, layout_hbm, out_ref,
    act, flipped, picked, lay, qb, kb, gb, send, held, vg, down_in, up_in, part, acc,
    act_sem, lay_sem, load_sem, swap_send, swap_recv, a2a_send, a2a_recv, ag_send, ag_recv,
    fwd_send, fwd_recv, rs_send, line_sem, end_sem, *, planes, inner,
):
    tokens, width = act_hbm.shape
    rows = out_ref.shape[0]
    bits = inner.bit_length() - 1
    me, core = lax.axis_index("dp"), lax.axis_index("seq")
    z, p = me // inner, me % inner
    other = 1 - core
    heads_cols, key_cols = q_hbm.shape[1] // SEQ, k_hbm.shape[1] // SEQ
    length = SEQ * tokens
    per_group = H // KVH
    groups = key_cols // HD
    half = rows // 2
    place = p * SEQ + core
    group_cols = per_group * HD
    stretches = [width // 8, width // 8] + [width // 4] * 3
    starts = [sum(stretches[:i]) for i in range(len(stretches))]

    cuts = ((k_hbm, kb, key_cols, 0, key_cols),) + tuple(
        (source, target, heads_cols, first, last - first)
        for first, last in ((0, group_cols), (group_cols, heads_cols))
        for source, target in ((q_hbm, qb), (grad_hbm, gb))
    )

    early_cuts = 3

    def cut(i, of_core):
        source, target, cols, first, count = cuts[i]
        return (
            source.at[:, pl.ds(pl.multiple_of(of_core * cols + first, 128), count)],
            target.at[pl.ds(pl.multiple_of(core * tokens, 128), tokens), pl.ds(first, count)],
        )

    flips = [
        pltpu.make_async_copy(
            act_hbm.at[:, pl.ds(at, count)],
            act.at[:, pl.ds(at, count)],
            act_sem.at[i],
        )
        for i, (at, count) in enumerate(zip(starts, stretches))
    ]
    lay_load = pltpu.make_async_copy(layout_hbm, lay, lay_sem)
    loads = [pltpu.make_async_copy(*cut(i, core), load_sem.at[int(i >= early_cuts)]) for i in range(len(cuts))]
    for load in [*flips, lay_load]:
        load.start()

    barrier = pltpu.get_barrier_semaphore()
    for j in range(1, inner * SEQ):
        to = (z * inner + relative(p, j // SEQ, bits), (core + j) % SEQ)
        pl.semaphore_signal(barrier, inc=1, device_id=to, device_id_type=MESH)

    @pl.when(z > 0)
    def _():
        pl.semaphore_signal(barrier, inc=1, device_id=(me - inner, core), device_id_type=MESH)

    @pl.when(z < planes - 1)
    def _():
        pl.semaphore_signal(barrier, inc=1, device_id=(me + inner, core), device_id_type=MESH)

    near = inner * SEQ - 1 + jnp.where(z > 0, 1, 0) + jnp.where(z < planes - 1, 1, 0)

    swaps = []
    for i in range(len(cuts)):
        source, target = cut(i, other)
        swaps.append(
            pltpu.make_async_remote_copy(
                src_ref=source, dst_ref=target, send_sem=swap_send, recv_sem=swap_recv.at[int(i >= early_cuts)],
                device_id=(me, other), device_id_type=MESH,
            )
        )
    for i, load in enumerate(flips):
        with jax.named_scope("act_wait"):
            load.wait()
        if i == 0:
            for other_load in loads:
                other_load.start()
        with jax.named_scope("flip"):
            at, count = starts[i], stretches[i]
            flipped[at : at + count, :] = act[:, at : at + count].T.astype(jnp.float32)
        if i == 2:
            with jax.named_scope("barrier"):
                pl.semaphore_wait(barrier, near)
            for swap in swaps:
                swap.start()
    lay_load.wait()

    def wait_for(like, sem):
        pltpu.make_async_remote_copy(
            src_ref=like, dst_ref=like, send_sem=sem, recv_sem=sem,
            device_id=(me, other), device_id_type=MESH,
        ).wait_recv()

    def pick(first_row):
        def some(i, carry):
            first = pl.multiple_of(i * 32, 32)
            for r in range(32):
                row = lay[first_row + first + r]
                picked[pl.ds(first + r, 1), :] = flipped[pl.ds(row, 1), :]
            return carry

        lax.fori_loop(0, half // 32, some, 0)

    def held_piece(owner, h):
        return held.at[
            owner,
            pl.ds(pl.multiple_of(h * half, 16), half),
            pl.ds(pl.multiple_of(place * tokens, 128), tokens),
        ]

    def block(k, h, j):
        to_p, to_core = relative(p, j // SEQ, bits), (core + j) % SEQ
        return pltpu.make_async_remote_copy(
            src_ref=send.at[k, j, pl.ds(pl.multiple_of(h * half, 16), half)],
            dst_ref=held_piece(turn(z, k, planes), h),
            send_sem=a2a_send,
            recv_sem=a2a_recv.at[k, h],
            device_id=(z * inner + to_p, to_core),
            device_id_type=MESH,
        )

    def gather(k, h):
        owner = turn(z, k, planes)

        def first_row(to_p, to_core):
            return ((owner * inner + to_p) * SEQ + to_core) * rows + h * half

        def to(i, carry):
            j = jnp.where(i <= 4, inner * SEQ - 1 - (i - 1) % 2 * 2 - (i - 1) // 2, inner * SEQ - i)
            pick(first_row(relative(p, j // SEQ, bits), (core + j) % SEQ))
            send[k, j, pl.ds(pl.multiple_of(h * half, 16), half)] = picked[...].astype(jnp.bfloat16)
            block(k, h, j).start()
            return carry

        lax.fori_loop(1, inner * SEQ, to, 0)
        pick(first_row(p, core))
        held_piece(owner, h)[...] = picked[...].astype(jnp.bfloat16)

    def took(k, h):
        wait_for(send.at[0, 1:, :half], a2a_recv.at[k, h])

    scale = math.log2(math.e) / float(HD) ** 0.5
    key_at = lax.broadcasted_iota(jnp.int32, (tokens, 2 * tokens), 0)
    query_at = lax.broadcasted_iota(jnp.int32, (tokens, 2 * tokens), 1) % tokens
    allowed = key_at <= query_at

    def weights_of(scores):
        powers = jnp.exp2((scores - jnp.max(scores, axis=0, keepdims=True)) * scale)
        return (powers * (1.0 / jnp.sum(powers, axis=0, keepdims=True))).astype(jnp.bfloat16)

    def stacked(ref, row, col):
        return jnp.concatenate(
            [
                ref[row : row + tokens, pl.ds(pl.multiple_of(col, 128), HD)],
                ref[row : row + tokens, pl.ds(pl.multiple_of(col + HD, 128), HD)],
            ],
            axis=0,
        )

    def grads(from_p, at):
        return vg.at[
            pl.ds(pl.multiple_of(from_p * length, 128), length),
            pl.ds(pl.multiple_of(at * HD, 128), HD),
        ]

    def attend(g):
        keys = kb[:, pl.ds(pl.multiple_of(g * HD, 128), HD)]
        early = jnp.zeros((tokens, HD), jnp.float32)
        both = jnp.zeros((length, HD), jnp.float32)
        for pair in range(per_group // 2):
            col = (g * per_group + 2 * pair) * HD
            against = (((1,), (1,)), ((), ()))
            first = lax.dot_general(
                keys[:tokens], stacked(qb, 0, col), against, preferred_element_type=jnp.float32
            )
            second = lax.dot_general(
                keys, stacked(qb, tokens, col), against, preferred_element_type=jnp.float32
            )
            first = jnp.where(allowed, first, -jnp.inf)
            second = jnp.concatenate(
                [second[:tokens], jnp.where(allowed, second[tokens:], -jnp.inf)], axis=0
            )
            early += jnp.dot(
                weights_of(first), stacked(gb, 0, col), preferred_element_type=jnp.float32
            )
            both += jnp.dot(
                weights_of(second), stacked(gb, tokens, col), preferred_element_type=jnp.float32
            )
        done = jnp.concatenate([both[:tokens] + early, both[tokens:]], axis=0)
        grads(p, 2 * g)[...] = done.astype(jnp.bfloat16)

    def gather_copy(g, jp):
        return pltpu.make_async_remote_copy(
            src_ref=grads(p, 2 * g), dst_ref=grads(p, 2 * g),
            send_sem=ag_send, recv_sem=ag_recv.at[g],
            device_id=(z * inner + relative(p, jp, bits), core), device_id_type=MESH,
        )

    def forward_copy(g, jp):
        from_p = relative(p, jp, bits)
        return pltpu.make_async_remote_copy(
            src_ref=grads(from_p, 2 * g), dst_ref=grads(from_p, 2 * g + 1),
            send_sem=fwd_send, recv_sem=fwd_recv.at[g],
            device_id=(me, other), device_id_type=MESH,
        )

    def publish(g):
        attend(g)
        for jp in reversed(range(1, inner)):
            gather_copy(g, jp).start()
        forward_copy(g, 0).start()

    def pass_on(g):
        wait_for(vg.at[: (inner - 1) * length, :HD], ag_recv.at[g])
        for jp in range(1, inner):
            forward_copy(g, jp).start()

    def arrived(g):
        wait_for(vg.at[:, :HD], fwd_recv.at[g])

    def slot(ref, owner, h, at, wide):
        count = rows if h is None else half
        first = 0 if h is None else pl.multiple_of(h * half, 16)
        return ref.at[owner, pl.ds(first, count), pl.ds(pl.multiple_of(at * HD, 128), wide * HD)]

    def end_sem_of(end, h, at):
        return end_sem.at[end, at if h is None or h == 0 else 2 * groups + at]

    def up_copy(owner, h, at, wide):
        sem = end_sem_of(1, h, at) if wide == 1 else line_sem.at[owner - 1, h, at // 2]
        return pltpu.make_async_remote_copy(
            src_ref=slot(part, owner, h, at, wide), dst_ref=slot(up_in, owner, h, at, wide),
            send_sem=rs_send, recv_sem=sem,
            device_id=(me + inner, core), device_id_type=MESH,
        )

    def down_copy(owner, h, at, wide, to):
        if wide == 1:
            sem = end_sem_of(0, h, at)
        else:
            sem = line_sem.at[jnp.where(owner == to, planes, owner) - 1 - jnp.where(owner == to, 1, 0), h, at // 2]
        return pltpu.make_async_remote_copy(
            src_ref=slot(part, owner, h, at, wide), dst_ref=slot(down_in, owner, h, at, wide),
            send_sem=rs_send, recv_sem=sem,
            device_id=(me - inner, core), device_id_type=MESH,
        )

    def reduce(k, h, at, wide):
        owner = turn(z, k, planes)
        count = rows if h is None else half
        at_rows = pl.ds(0 if h is None else pl.multiple_of(h * half, 16), count)
        cols = pl.ds(pl.multiple_of(at * HD, 128), wide * HD)
        here = acc.at[:count, : wide * HD]
        here[...] = jnp.dot(held[owner, at_rows, :], vg[:, cols], preferred_element_type=jnp.float32)

        @pl.when((owner >= z) & (z > 0))
        def _():
            up_copy(owner, h, at, wide).wait_recv()
            here[...] += slot(up_in, owner, h, at, wide)[...].astype(jnp.float32)

        @pl.when((owner <= z) & (z < planes - 1))
        def _():
            down_copy(owner, h, at, wide, z).wait_recv()
            here[...] += slot(down_in, owner, h, at, wide)[...].astype(jnp.float32)

        @pl.when(owner == z)
        def _():
            for c in range(wide):
                of_core = (core + at + c) % SEQ
                out_ref[at_rows, pl.ds(pl.multiple_of((of_core * groups + (at + c) // 2) * HD, 128), HD)] = acc[
                    :count, c * HD : (c + 1) * HD
                ]

        @pl.when(owner != z)
        def _():
            slot(part, owner, h, at, wide)[...] = here[...].astype(jnp.bfloat16)

        @pl.when(owner > z)
        def _():
            up_copy(owner, h, at, wide).start()

        @pl.when(owner < z)
        def _():
            down_copy(owner, h, at, wide, z - 1).start()

    def reduce_both(k):
        each(0, 2, lambda at: [reduce(k, h, at, 1) for h in range(2)])
        each(2, 2 * groups, lambda at: reduce(k, None, at, 1))

    def at_end(k):
        owner = turn(z, k, planes)
        return (owner == 0) | (owner == planes - 1)

    def each(first, last, step):
        lax.fori_loop(first, last, lambda i, carry: (step(i), carry)[1], 0)

    with jax.named_scope("g00"):
        gather(0, 0)
    with jax.named_scope("qwait"):
        for sem in (load_sem, swap_recv):
            wait_for(qb.at[:tokens, : 2 * group_cols + key_cols], sem.at[0])
    with jax.named_scope("a0"):
        publish(0)
    with jax.named_scope("g01"):
        gather(0, 1)
    with jax.named_scope("qwait2"):
        for sem in (load_sem, swap_recv):
            wait_for(qb.at[:, group_cols:], sem.at[1])
    with jax.named_scope("a123"):
        each(1, groups, publish)
    later = [lambda i=i: gather(i // 2, i % 2) for i in range(2, 2 * planes)]

    def next_gather():
        if later:
            with jax.named_scope("gnext"):
                later.pop(0)()

    for g in range(groups):
        with jax.named_scope(f"pass{g}"):
            pass_on(g)
        if g == 0:
            with jax.named_scope("took00"):
                took(0, 0)
        with jax.named_scope(f"red0_{g}own"):
            reduce(0, None if g else 0, 2 * g, 1)
        if g == 0:
            next_gather()
        with jax.named_scope(f"arr{g}"):
            arrived(g)
        with jax.named_scope(f"red0_{g}other"):
            reduce(0, None if g else 0, 2 * g + 1, 1)
            if g == 0:
                with jax.named_scope("took01"):
                    took(0, 1)
                reduce(0, 1, 0, 1)
                reduce(0, 1, 1, 1)
        if g == 0:
            next_gather()
        if g < groups - 1:
            next_gather()

    def rest(k, between=None):
        def half_of(h):
            with jax.named_scope("took"):
                took(k, h)

            @pl.when(jnp.logical_not(at_end(k)))
            def _():
                with jax.named_scope("red"):
                    each(0, groups, lambda g: reduce(k, h, 2 * g, 2))

        half_of(0)
        if between is not None:
            between()
        half_of(1)

        @pl.when(at_end(k))
        def _():
            with jax.named_scope("redend"):
                reduce_both(k)

    rest(1, lambda: each(2 * planes - len(later), 2 * planes, lambda i: gather(i // 2, i % 2)))
    each(2, planes, rest)

    with jax.named_scope("t0"):
        for ref in (qb, gb, kb):
            wait_for(ref.at[:tokens], swap_send)
        wait_for(send.at[:, 1:], a2a_send)
        wait_for(vg.at[: (inner - 1) * length, : groups * HD], ag_send)
        wait_for(vg.at[:, : groups * HD], fwd_send)
    with jax.named_scope("t3"):
        wait_for(part.at[1:], rs_send)


def body(activations, queries, keys, out_grad, layout):
    members = lax.axis_size("dp")
    tokens, width = activations.shape
    inner = 1 << ((members.bit_length() - 1) // 2)
    planes = members // inner
    rows = layout.shape[0] // (members * SEQ)
    kv_width = keys.shape[1]
    groups = kv_width // SEQ // HD
    length = SEQ * tokens
    dma = pltpu.SemaphoreType.DMA
    operands = (activations, queries, keys, out_grad, layout)
    return pl.pallas_call(
        functools.partial(fused_kernel, planes=planes, inner=inner),
        out_shape=jax.ShapeDtypeStruct((rows, kv_width), jnp.float32),
        in_specs=[pl.BlockSpec(memory_space=pltpu.HBM)] * len(operands),
        out_specs=pl.BlockSpec(memory_space=pltpu.VMEM),
        scratch_shapes=[
            pltpu.VMEM((tokens, width), jnp.bfloat16),
            pltpu.VMEM((width, tokens), jnp.float32),
            pltpu.VMEM((rows // 2, tokens), jnp.float32),
            pltpu.SMEM(layout.shape, jnp.int32),
            pltpu.VMEM((length, queries.shape[1] // SEQ), jnp.bfloat16),
            pltpu.VMEM((length, kv_width // SEQ), jnp.bfloat16),
            pltpu.VMEM((length, queries.shape[1] // SEQ), jnp.bfloat16),
            pltpu.VMEM((planes, inner * SEQ, rows, tokens), jnp.bfloat16),
            pltpu.VMEM((planes, rows, inner * length), jnp.bfloat16),
            pltpu.VMEM((inner * length, kv_width), jnp.bfloat16),
            pltpu.VMEM((planes, rows, kv_width), jnp.bfloat16),
            pltpu.VMEM((planes, rows, kv_width), jnp.bfloat16),
            pltpu.VMEM((planes, rows, kv_width), jnp.bfloat16),
            pltpu.VMEM((rows, SEQ * HD), jnp.float32),
            dma((5,)),
            dma(()),
            dma((2,)),
            dma(()),
            dma((2,)),
            dma(()),
            dma((planes, 2)),
            dma(()),
            dma((groups,)),
            dma(()),
            dma((groups,)),
            dma(()),
            dma((planes - 1, 2, groups)),
            dma((2, 2 * groups + 2)),
        ],
        compiler_params=pltpu.CompilerParams(
            collective_id=0, has_side_effects=True, vmem_limit_bytes=32 * 2**20
        ),
    )(*(pltpu.with_memory_space_constraint(x, pltpu.HBM) for x in operands))


def solution(mesh):
    whole = ("dp", "seq")
    return jax.shard_map(
        body,
        mesh=mesh,
        in_specs=(P(whole, None),) * 4 + (P(),),
        out_specs=P(whole, None),
        check_vma=False,
    )
```
